32 devices in a mesh: fsdp: 16 (over z, y, x), rep: 2 (over core).
Axes of the slice: x: 2, y: 2, z: 4, core: 2. Of those that a mesh axis runs over, the one named last changes fastest.
Arguments:
- captions: bfloat16 [320, 128, 768], P(('fsdp', 'rep')), may hold values from -6 to 6
- regions: bfloat16 [64, 128, 768], P(('fsdp', 'rep')), may hold values from -6 to 6
- caption_lengths: int32 [320], P(('fsdp', 'rep')), may hold values from 64 to 128, as said below
- region_counts: int32 [64], P(('fsdp', 'rep')), may hold values from 36 to 100, as said below
- group_ids: int32 [320], P(('fsdp', 'rep')), may hold values from 0 to 1, as said below
- query_weight: bfloat16 [768, 768], P('fsdp'), may hold values from -0.21875 to 0.21875
- key_weight: bfloat16 [768, 768], P('fsdp'), may hold values from -0.21875 to 0.21875
- value_weight: bfloat16 [768, 768], P('fsdp'), may hold values from -0.21875 to 0.21875
- out_weight: bfloat16 [768, 768], P('fsdp'), may hold values from -1.5 to 1.5
- query_bias: bfloat16 [768], P('fsdp'), may hold values from -3 to 3
- value_bias: bfloat16 [768], P('fsdp'), may hold values from -3 to 3
- out_bias: bfloat16 [768], P('fsdp'), may hold values from -3 to 3
- first_gain: bfloat16 [768], P('fsdp'), may hold values from 0.25 to 1.75
- first_shift: bfloat16 [768], P('fsdp'), may hold values from -3 to 3
- inner_weight: bfloat16 [768, 3072], P('fsdp'), may hold values from -0.21875 to 0.21875
- inner_bias: bfloat16 [3072], P('fsdp'), may hold values from -3 to 3
- outer_weight: bfloat16 [3072, 768], P('fsdp'), may hold values from -0.109375 to 0.109375
- outer_bias: bfloat16 [768], P('fsdp'), may hold values from -3 to 3
- second_gain: bfloat16 [768], P('fsdp'), may hold values from 0.25 to 1.75
- second_shift: bfloat16 [768], P('fsdp'), may hold values from -3 to 3
- caption_cotangent: bfloat16 [320, 128, 768], P(('fsdp', 'rep')), may hold values from -6 to 6
- region_cotangent: bfloat16 [320, 128, 768], P(('fsdp', 'rep')), may hold values from -6 to 6
Outputs:
- out_caption: bfloat16 [320, 128, 768], P(('fsdp', 'rep'))
- out_region: bfloat16 [320, 128, 768], P(('fsdp', 'rep'))
- grad_captions: float32 [320, 128, 768], P(('fsdp', 'rep'))
- grad_regions: float32 [64, 128, 768], P(('fsdp', 'rep'))
- query_weight_grad: float32 [768, 768], P('fsdp')
- key_weight_grad: float32 [768, 768], P('fsdp')
- value_weight_grad: float32 [768, 768], P('fsdp')
- out_weight_grad: float32 [768, 768], P('fsdp')
- query_bias_grad: float32 [768], P('fsdp')
- value_bias_grad: float32 [768], P('fsdp')
- out_bias_grad: float32 [768], P('fsdp')
- first_gain_grad: float32 [768], P('fsdp')
- first_shift_grad: float32 [768], P('fsdp')
- inner_weight_grad: float32 [768, 3072], P('fsdp')
- inner_bias_grad: float32 [3072], P('fsdp')
- outer_weight_grad: float32 [3072, 768], P('fsdp')
- outer_bias_grad: float32 [768], P('fsdp')
- second_gain_grad: float32 [768], P('fsdp')
- second_shift_grad: float32 [768], P('fsdp')
The draws below stay inside these ranges and needn't reach their ends.
Inputs may be any that keep to these rules, and one draw needn't show every extreme that they name: `caption_lengths`: the slots of a caption past its length are padding; some caption reaches 128. `region_counts`: the slots of an image past its count are padding; some image reaches 100. Sequence s uses image (s // 10) * 2 + group_ids[s]; every image is used by exactly five sequences.
All inputs are finite; a program needn't handle non-finite values.
Results may differ from the reference program's by a relative error of at most 0.015.
Values may be sent and summed in bfloat16 or wider, within the bound.
A program may use at most 320 MiB of HBM per device.

```python
import jax
import jax.numpy as jnp
from jax import lax

D = 768
HEADS = 12
HEAD = 64
FF = 3072
CAP = 128
RMAX = 128
CAP_LEAST = 64
REG_LEAST = 36
REG_MOST = 100
SEQ_DEV = 10
IMG_DEV = 2
LEN = 256
SEQS = 320
IMAGES = 64


def draw_caption_lengths(key, part):
    first_key, second_key = jax.random.split(key)
    drawn = jax.random.randint(first_key, (SEQS,), CAP_LEAST, CAP + 1)
    longest = jax.random.randint(second_key, (), 0, SEQS)
    return drawn.at[longest].set(CAP).astype(jnp.int32)


def draw_region_counts(key, part):
    first_key, second_key = jax.random.split(key)
    drawn = jax.random.randint(first_key, (IMAGES,), REG_LEAST, REG_MOST + 1)
    longest = jax.random.randint(second_key, (), 0, IMAGES)
    return drawn.at[longest].set(REG_MOST).astype(jnp.int32)


def draw_group_ids(key, part):
    block_keys = jax.random.split(key, SEQS // SEQ_DEV)
    numbered = jnp.repeat(jnp.arange(IMG_DEV, dtype=jnp.int32), SEQ_DEV // IMG_DEV)

    def block_draw(block_key):
        return jax.random.permutation(block_key, numbered)
    return jax.vmap(block_draw)(block_keys).reshape(SEQS).astype(jnp.int32)


def levels(rng, shape, cuts, low, largest):
    gain, own = 1.0, jax.random.fold_in(rng, 6)
    for dim, parts in cuts:
        heights = jnp.exp(jax.random.uniform(jax.random.fold_in(own, dim), (parts,), jnp.float32, low / len(cuts), largest / len(cuts)))
        gain = gain * jnp.repeat(heights, shape[dim] // parts).reshape([-1 if axis == dim else 1 for axis in range(len(shape))])
    return gain


def normal_values(key, dims, scale, reach, cuts=(), kind=jnp.bfloat16):
    values = jax.random.normal(key, dims, jnp.float32) * scale
    if len(cuts) > 0:
        values = levels(key, dims, cuts, -0.22, 0.18) * values
    return jnp.clip(values, min=-reach, max=reach).astype(kind)


def setup_inputs(seed: int = 0) -> dict:
    streams_of = jax.random.split(jax.random.key(seed), 23)
    return {
        "captions": normal_values(streams_of[0], (SEQS, CAP, D), 1.0, 6.0, ((0, 32),)),
        "regions": normal_values(streams_of[1], (IMAGES, RMAX, D), 1.0, 6.0, ((0, 32),)),
        "caption_lengths": draw_caption_lengths(jax.random.fold_in(streams_of[22], 71), 0),
        "region_counts": draw_region_counts(jax.random.fold_in(streams_of[22], 71), 0),
        "group_ids": draw_group_ids(jax.random.fold_in(streams_of[22], 71), 0),
        "query_weight": normal_values(streams_of[5], (D, D), D ** -0.5, 0.21875, ((0, 16),)),
        "key_weight": normal_values(streams_of[6], (D, D), D ** -0.5, 0.21875, ((0, 16),)),
        "value_weight": normal_values(streams_of[7], (D, D), D ** -0.5, 0.21875, ((0, 16),)),
        "out_weight": normal_values(streams_of[8], (D, D), (HEAD // 4) ** -0.5, 1.5, ((0, 16),)),
        "query_bias": normal_values(streams_of[9], (D,), 0.5, 3.0, ((0, 16),)),
        "value_bias": normal_values(streams_of[10], (D,), 0.5, 3.0, ((0, 16),)),
        "out_bias": normal_values(streams_of[11], (D,), 0.5, 3.0, ((0, 16),)),
        "first_gain": jnp.clip(1.0 + 0.15 * jax.random.normal(streams_of[12], (D,), jnp.float32), 0.25, 1.75).astype(jnp.bfloat16),
        "first_shift": normal_values(streams_of[13], (D,), 0.5, 3.0, ((0, 16),)),
        "inner_weight": normal_values(streams_of[14], (D, FF), D ** -0.5, 0.21875, ((0, 16),)),
        "inner_bias": normal_values(streams_of[15], (FF,), 0.5, 3.0, ((0, 16),)),
        "outer_weight": normal_values(streams_of[16], (FF, D), FF ** -0.5, 0.109375, ((0, 16),)),
        "outer_bias": normal_values(streams_of[17], (D,), 0.5, 3.0, ((0, 16),)),
        "second_gain": jnp.clip(1.0 + 0.15 * jax.random.normal(streams_of[18], (D,), jnp.float32), 0.25, 1.75).astype(jnp.bfloat16),
        "second_shift": normal_values(streams_of[19], (D,), 0.5, 3.0, ((0, 16),)),
        "caption_cotangent": normal_values(streams_of[20], (SEQS, CAP, D), 1.0, 6.0, ((0, 32),)),
        "region_cotangent": normal_values(streams_of[21], (SEQS, RMAX, D), 1.0, 6.0, ((0, 32),)),
    }


EPSILON = 1e-12
MASKED_SCORE = -1e+30
HIGHEST_PRECISION = lax.Precision.HIGHEST

@jax.custom_vjp
def low(v):
    return lax.optimization_barrier(v.astype(jnp.bfloat16)).astype(jnp.float32)

@jax.custom_vjp
def low_back(v):
    return v

def low_keep(v):
    return (low(v), None)

def low_pass(kept, grad):
    return (grad,)

def back_keep(v):
    return (v, None)

def back_low(kept, grad):
    return (low(grad),)
low.defvjp(low_keep, low_pass)
low_back.defvjp(back_keep, back_low)

def normalize(values, norm_gain, norm_shift):
    average = lax.optimization_barrier(jnp.mean(values, axis=-1, keepdims=True))
    centred = values - average
    spread = lax.optimization_barrier(jnp.mean(centred * centred, axis=-1, keepdims=True))
    return centred * lax.rsqrt(spread + EPSILON) * norm_gain + norm_shift

def matmul_high(left, right):
    return jnp.matmul(left, right, precision=HIGHEST_PRECISION)

def one_block(weight_set, captions, regions, caption_lengths, region_counts, group_ids):
    query_weight, key_weight, value_weight, out_weight, query_bias, value_bias, out_bias, first_gain, first_shift, inner_weight, inner_bias, outer_weight, outer_bias, second_gain, second_shift = weight_set
    seq_count = captions.shape[0]

    def with_bias(row_block, weight, bias_vec):
        return low_back(low(matmul_high(row_block, weight) + bias_vec))

    def without_bias(row_block, weight):
        return low_back(low(matmul_high(row_block, weight)))

    def sequence_rows(caption_part, image_part):
        return jnp.concatenate([caption_part, jnp.take(image_part, group_ids, axis=0)], axis=1)
    queries = sequence_rows(with_bias(captions, query_weight, query_bias), with_bias(regions, query_weight, query_bias)).reshape(seq_count, LEN, HEADS, HEAD)
    keys_seq = sequence_rows(without_bias(captions, key_weight), without_bias(regions, key_weight)).reshape(seq_count, LEN, HEADS, HEAD)
    values_seq = sequence_rows(with_bias(captions, value_weight, value_bias), with_bias(regions, value_weight, value_bias)).reshape(seq_count, LEN, HEADS, HEAD)
    caption_live = jnp.arange(CAP)[None, :] < caption_lengths[:, None]
    region_live = jnp.arange(RMAX)[None, :] < jnp.take(region_counts, group_ids)[:, None]
    live_rows = jnp.concatenate([caption_live, region_live], axis=1)
    products = jnp.einsum('sqhe,skhe->shqk', queries, keys_seq, precision=HIGHEST_PRECISION)
    scores = low_back(products * HEAD ** (-0.5))
    scores = jnp.where(live_rows[:, None, None, :], scores, MASKED_SCORE)
    soft_low = low(jax.nn.softmax(scores, axis=-1))
    context = jnp.einsum('shqk,skhe->sqhe', soft_low, values_seq, precision=HIGHEST_PRECISION)
    context = low_back(low(context.reshape(seq_count, LEN, D)))
    attended = low_back(matmul_high(context, out_weight) + out_bias)
    inputs_seq = sequence_rows(captions, regions)
    first_out = normalize(inputs_seq + attended, first_gain, first_shift)
    inner_pre = low_back(matmul_high(low(first_out), inner_weight) + inner_bias)
    active_low = low(jax.nn.gelu(inner_pre, approximate=False))
    outer_out = low_back(matmul_high(active_low, outer_weight) + outer_bias)
    layer_out = normalize(first_out + outer_out, second_gain, second_shift)
    return layer_out * live_rows[:, :, None].astype(jnp.float32)

def reference(captions, regions, caption_lengths, region_counts, group_ids, query_weight, key_weight, value_weight, out_weight, query_bias, value_bias, out_bias, first_gain, first_shift, inner_weight, inner_bias, outer_weight, outer_bias, second_gain, second_shift, caption_cotangent, region_cotangent):
    block_count = SEQS // SEQ_DEV
    weight_set = (query_weight.astype(jnp.float32), key_weight.astype(jnp.float32), value_weight.astype(jnp.float32), out_weight.astype(jnp.float32), query_bias.astype(jnp.float32), value_bias.astype(jnp.float32), out_bias.astype(jnp.float32), first_gain.astype(jnp.float32), first_shift.astype(jnp.float32), inner_weight.astype(jnp.float32), inner_bias.astype(jnp.float32), outer_weight.astype(jnp.float32), outer_bias.astype(jnp.float32), second_gain.astype(jnp.float32), second_shift.astype(jnp.float32))
    caption_blocks = captions.astype(jnp.float32).reshape(block_count, SEQ_DEV, CAP, D)
    region_blocks = regions.astype(jnp.float32).reshape(block_count, IMG_DEV, RMAX, D)
    length_blocks = caption_lengths.reshape(block_count, SEQ_DEV)
    count_blocks = region_counts.reshape(block_count, IMG_DEV)
    group_blocks = group_ids.reshape(block_count, SEQ_DEV)
    block_function = jax.checkpoint(one_block)

    def forward(weights_now, caption_now, region_now):

        def scan_step(scan_carry, scan_item):
            cap_item, reg_item, len_item, count_item, group_item = scan_item
            return (scan_carry, block_function(weights_now, cap_item, reg_item, len_item, count_item, group_item))
        return lax.scan(scan_step, jnp.zeros((), jnp.float32), (caption_now, region_now, length_blocks, count_blocks, group_blocks))[1]
    layer_out, pullback = jax.vjp(forward, weight_set, caption_blocks, region_blocks)
    cotangent = jnp.concatenate([caption_cotangent.astype(jnp.float32).reshape(block_count, SEQ_DEV, CAP, D), region_cotangent.astype(jnp.float32).reshape(block_count, SEQ_DEV, RMAX, D)], axis=2)
    weight_grads, caption_grad, region_grad = pullback(cotangent)
    query_weight_grad, key_weight_grad, value_weight_grad, out_weight_grad, query_bias_grad, value_bias_grad, out_bias_grad, first_gain_grad, first_shift_grad, inner_weight_grad, inner_bias_grad, outer_weight_grad, outer_bias_grad, second_gain_grad, second_shift_grad = weight_grads
    out_caption = layer_out[:, :, :CAP].reshape(SEQS, CAP, D).astype(jnp.bfloat16)
    out_region = layer_out[:, :, CAP:].reshape(SEQS, RMAX, D).astype(jnp.bfloat16)
    return (out_caption, out_region, caption_grad.reshape(SEQS, CAP, D), region_grad.reshape(IMAGES, RMAX, D), query_weight_grad, key_weight_grad, value_weight_grad, out_weight_grad, query_bias_grad, value_bias_grad, out_bias_grad, first_gain_grad, first_shift_grad, inner_weight_grad, inner_bias_grad, outer_weight_grad, outer_bias_grad, second_gain_grad, second_shift_grad)
```

```python
import functools

import jax
import jax.numpy as jnp
from jax import lax
from jax.experimental import pallas as pl
from jax.experimental.pallas import tpu as pltpu
from jax.sharding import PartitionSpec as P

HEADS = 12


EPSILON = 1e-12
MASKED_SCORE = -1e30
HIGHEST_PRECISION = lax.Precision.HIGHEST


def normalize(values, norm_gain, norm_shift):
    average = jnp.mean(values, axis=-1, keepdims=True)
    centred = values - average
    spread = jnp.mean(centred * centred, axis=-1, keepdims=True)
    return centred * lax.rsqrt(spread + EPSILON) * norm_gain + norm_shift


def exact_gelu(values):
    return jax.nn.gelu(values, approximate=False)


def forward_rows(row_block, weight):
    return jnp.dot(row_block, weight, preferred_element_type=jnp.float32)


def backward_rows(gradient, weight):
    return lax.dot_general(
        gradient, weight, (((1,), (1,)), ((), ())), preferred_element_type=jnp.float32
    )


def weight_grad(row_block, gradient):
    return lax.dot_general(
        row_block, gradient, (((0,), (0,)), ((), ())), preferred_element_type=jnp.float32
    )


def column_sum(gradient):
    return jnp.sum(gradient.astype(jnp.float32), axis=0)


MESH = pl.DeviceIdType.MESH
PLANES = 4
COLUMN_SPLIT, ROW_SPLIT = 0, 1


def place_of(index, half, step, first, second):
    across = first * (1 - half) + second * half
    down = second * (1 - half) + first * half
    plane = lax.rem(index // 4 + step, PLANES)
    row = lax.rem(lax.rem(index // 2, 2) + down, 2)
    column = lax.rem(lax.rem(index, 2) + across, 2)
    return plane * 4 + row * 2 + column


def part_of(ref, split, owner, half, count, align):
    rows, columns = ref.shape[0] // count, ref.shape[1]
    if split == COLUMN_SPLIT:
        width = columns // 2
        return ref.at[
            pl.ds(pl.multiple_of(owner * rows, align), rows),
            pl.ds(pl.multiple_of(half * width, 128), width),
        ]
    height = rows // 2
    return ref.at[pl.ds(pl.multiple_of(owner * rows + half * height, align), height)]


def greet(index, half):
    barrier = pltpu.get_barrier_semaphore()
    peers = [(place_of(index, half, step, 0, 0), half) for step in (1, 2, 3)]
    peers += [(place_of(index, half, 0, 1, 0), half), (place_of(index, half, 0, 0, 1), half)]
    peers += [(index, 1 - half)]
    for peer in peers:
        pl.semaphore_signal(barrier, inc=1, device_id=peer, device_id_type=MESH)
    pl.semaphore_wait(barrier, len(peers))


def gather_kernel(splits, aligns, *refs):
    count = len(splits)
    shards, wholes = refs[:count], refs[count : 2 * count]
    (own_sem, z_send, z_recv, a_send, a_recv, b_send, b_recv, s_send, s_recv) = refs[2 * count :]
    index, half = lax.axis_index("fsdp"), lax.axis_index("rep")
    owners = wholes[0].shape[0] // shards[0].shape[0]

    def owner_of(step, first, second):
        return place_of(index, half, step, first, second)

    def piece(tensor, step, first, second):
        owner = owner_of(step, first, second)
        return part_of(wholes[tensor], splits[tensor], owner, half, owners, aligns[tensor])

    def copy_piece(tensor, source, step, first, second, send, recv, peer):
        return pltpu.make_async_remote_copy(
            src_ref=source,
            dst_ref=piece(tensor, step, first, second),
            send_sem=send,
            recv_sem=recv,
            device_id=peer,
            device_id_type=MESH,
        )

    peer_a = (owner_of(0, 1, 0), half)
    peer_b = (owner_of(0, 0, 1), half)
    sibling = (index, 1 - half)

    def to_z(tensor, source, hop):
        peer = (owner_of(hop, 0, 0), half)
        slot = PLANES - hop - 1
        return copy_piece(
            tensor, source, 0, 0, 0, z_send.at[tensor, hop - 1], z_recv.at[tensor, slot], peer
        )

    def to_a(tensor, source, step):
        return copy_piece(
            tensor, source, step, 0, 0, a_send.at[tensor, step], a_recv.at[tensor, step], peer_a
        )

    def to_b(tensor, source, step, first):
        slot = step * 2 + first
        return copy_piece(
            tensor, source, step, first, 0, b_send.at[tensor, slot], b_recv.at[tensor, slot], peer_b
        )

    def to_sibling(tensor, source, step, first, second):
        slot = step * 4 + first * 2 + second - 1
        return copy_piece(
            tensor,
            source,
            step,
            first,
            second,
            s_send.at[tensor, slot],
            s_recv.at[tensor, slot],
            sibling,
        )

    greet(index, half)
    started = []
    local = []
    for tensor in range(count):
        shard = shards[tensor]
        rows = shard.shape[0]
        source = part_of(shard, splits[tensor], 0, half, 1, aligns[tensor])
        sends = [to_z(tensor, source, hop) for hop in (1, 2, 3)]
        sends += [to_a(tensor, source, 0), to_b(tensor, source, 0, 0)]
        for copy in sends:
            copy.start()
        started += sends
        here = pltpu.make_async_copy(
            shard,
            wholes[tensor].at[pl.ds(pl.multiple_of(index * rows, aligns[tensor]), rows)],
            own_sem.at[tensor],
        )
        here.start()
        local.append(here)
    for tensor in range(count):
        for step in (1, 2, 3):
            source = piece(tensor, step, 0, 0)
            copy_piece(
                tensor,
                source,
                step,
                0,
                0,
                z_send.at[tensor, step - 1],
                z_recv.at[tensor, step - 1],
                sibling,
            ).wait_recv()
            sends = [
                to_b(tensor, source, step, 0),
                to_a(tensor, source, step),
                to_sibling(tensor, source, step, 0, 0),
            ]
            for copy in sends:
                copy.start()
            started += sends
    for tensor in range(count):
        for step in range(PLANES):
            source = piece(tensor, step, 1, 0)
            copy_piece(
                tensor,
                source,
                step,
                1,
                0,
                a_send.at[tensor, step],
                a_recv.at[tensor, step],
                peer_a,
            ).wait_recv()
            sends = [to_b(tensor, source, step, 1), to_sibling(tensor, source, step, 1, 0)]
            for copy in sends:
                copy.start()
            started += sends
    for tensor in range(count):
        for step in range(PLANES):
            for first in (0, 1):
                source = piece(tensor, step, first, 1)
                slot = step * 2 + first
                copy_piece(
                    tensor,
                    source,
                    step,
                    first,
                    1,
                    b_send.at[tensor, slot],
                    b_recv.at[tensor, slot],
                    peer_b,
                ).wait_recv()
                copy = to_sibling(tensor, source, step, first, 1)
                copy.start()
                started.append(copy)
    for tensor in range(count):
        local[tensor].wait()
        for step in range(PLANES):
            for first in (0, 1):
                for second in (0, 1):
                    if step + first + second == 0:
                        continue
                    slot = step * 4 + first * 2 + second - 1
                    owner = place_of(index, 1 - half, step, first, second)
                    there = part_of(
                        wholes[tensor], splits[tensor], owner, 1 - half, owners, aligns[tensor]
                    )
                    pltpu.make_async_remote_copy(
                        src_ref=there,
                        dst_ref=there,
                        send_sem=s_send.at[tensor, slot],
                        recv_sem=s_recv.at[tensor, slot],
                        device_id=sibling,
                        device_id_type=MESH,
                    ).wait_recv()
    for copy in started:
        copy.wait_send()


def gather_all(shards, splits, owners, collective_id):
    count = len(shards)
    aligns = [16 if shard.dtype == jnp.bfloat16 else 8 for shard in shards]
    dma = pltpu.SemaphoreType.DMA
    return pl.pallas_call(
        functools.partial(gather_kernel, splits, aligns),
        out_shape=[
            jax.ShapeDtypeStruct((owners * shard.shape[0], shard.shape[1]), shard.dtype)
            for shard in shards
        ],
        in_specs=[pl.BlockSpec(memory_space=pltpu.VMEM)] * count,
        out_specs=[pl.BlockSpec(memory_space=pl.ANY)] * count,
        scratch_shapes=[
            dma((count,)),
            dma((count, 3)),
            dma((count, 3)),
            dma((count, 4)),
            dma((count, 4)),
            dma((count, 8)),
            dma((count, 8)),
            dma((count, 15)),
            dma((count, 15)),
        ],
        compiler_params=pltpu.CompilerParams(collective_id=collective_id, has_side_effects=True),
        name="gather_rows",
    )(*shards)


def reduce_kernel(splits, aligns, owners, *refs):
    count = len(splits)
    partials, totals = refs[:count], refs[count : 2 * count]
    mine = refs[2 * count : 3 * count]
    core_in = refs[3 * count : 4 * count]
    b_in = refs[4 * count : 5 * count]
    a_in = refs[5 * count : 6 * count]
    z_in = refs[6 * count : 7 * count]
    (load_sem, c_send, c_recv, b_send, b_recv, a_send, a_recv, z_send, z_recv, o_send, o_recv) = (
        refs[7 * count :]
    )
    index, half = lax.axis_index("fsdp"), lax.axis_index("rep")
    sibling = (index, 1 - half)
    peer_a = (place_of(index, half, 0, 1, 0), half)
    peer_b = (place_of(index, half, 0, 0, 1), half)

    def slot_of(step, first, second):
        return second * 8 + first * 4 + step

    def load(tensor, step, first, second):
        owner = place_of(index, half, step, first, second)
        slot = slot_of(step, first, second)
        return pltpu.make_async_copy(
            part_of(partials[tensor], splits[tensor], owner, half, owners, aligns[tensor]),
            mine[tensor].at[slot],
            load_sem.at[tensor, slot],
        )

    def to_core(tensor, step, first, second):
        owner = place_of(index, 1 - half, step, first, second)
        slot = slot_of(step, first, second)
        return pltpu.make_async_remote_copy(
            src_ref=part_of(
                partials[tensor], splits[tensor], owner, 1 - half, owners, aligns[tensor]
            ),
            dst_ref=core_in[tensor].at[slot],
            send_sem=c_send.at[tensor, slot],
            recv_sem=c_recv.at[tensor, slot],
            device_id=sibling,
            device_id_type=MESH,
        )

    def to_b(tensor, step, first):
        slot = first * 4 + step
        return pltpu.make_async_remote_copy(
            src_ref=mine[tensor].at[8 + slot],
            dst_ref=b_in[tensor].at[slot],
            send_sem=b_send.at[tensor, slot],
            recv_sem=b_recv.at[tensor, slot],
            device_id=peer_b,
            device_id_type=MESH,
        )

    def to_a(tensor, step):
        return pltpu.make_async_remote_copy(
            src_ref=mine[tensor].at[4 + step],
            dst_ref=a_in[tensor].at[step],
            send_sem=a_send.at[tensor, step],
            recv_sem=a_recv.at[tensor, step],
            device_id=peer_a,
            device_id_type=MESH,
        )

    def to_z(tensor, hop):
        return pltpu.make_async_remote_copy(
            src_ref=mine[tensor].at[hop],
            dst_ref=z_in[tensor].at[PLANES - hop - 1],
            send_sem=z_send.at[tensor, hop - 1],
            recv_sem=z_recv.at[tensor, PLANES - hop - 1],
            device_id=(place_of(index, half, hop, 0, 0), half),
            device_id_type=MESH,
        )

    def wide(ref):
        return ref[...].astype(jnp.float32)

    def output_part(tensor):
        return part_of(totals[tensor], splits[tensor], 0, half, 1, 8)

    def to_output(tensor):
        return pltpu.make_async_remote_copy(
            src_ref=output_part(tensor),
            dst_ref=output_part(tensor),
            send_sem=o_send.at[tensor],
            recv_sem=o_recv.at[tensor],
            device_id=sibling,
            device_id_type=MESH,
        )

    greet(index, half)

    order = [(step, first, 1) for first in (1, 0) for step in (1, 2, 3, 0)]
    order += [(step, 1, 0) for step in (1, 2, 3, 0)] + [(step, 0, 0) for step in (1, 2, 3, 0)]
    for tensor in range(count):
        for step, first, second in order:
            to_core(tensor, step, first, second).start()
            load(tensor, step, first, second).start()

    for tensor in range(count):

        def b_step(turn, carry, tensor=tensor):
            step, first = lax.rem(turn + 1, PLANES), 1 - turn // PLANES
            load(tensor, step, first, 1).wait()
            to_core(tensor, step, first, 1).wait_recv()
            slot = slot_of(step, first, 1)
            total = wide(mine[tensor].at[slot]) + wide(core_in[tensor].at[slot])
            mine[tensor].at[slot][...] = total.astype(mine[tensor].dtype)
            to_b(tensor, step, first).start()
            return carry

        lax.fori_loop(0, 2 * PLANES, b_step, 0)
    for tensor in range(count):

        def a_step(turn, carry, tensor=tensor):
            step = lax.rem(turn + 1, PLANES)
            load(tensor, step, 1, 0).wait()
            to_core(tensor, step, 1, 0).wait_recv()
            to_b(tensor, step, 1).wait_recv()
            slot = slot_of(step, 1, 0)
            total = wide(mine[tensor].at[slot]) + wide(core_in[tensor].at[slot])
            total += wide(b_in[tensor].at[slot])
            mine[tensor].at[slot][...] = total.astype(mine[tensor].dtype)
            to_a(tensor, step).start()
            return carry

        lax.fori_loop(0, PLANES, a_step, 0)
    for tensor in range(count):

        def total_of(step, tensor=tensor):
            load(tensor, step, 0, 0).wait()
            to_core(tensor, step, 0, 0).wait_recv()
            to_b(tensor, step, 0).wait_recv()
            to_a(tensor, step).wait_recv()
            total = wide(mine[tensor].at[step]) + wide(core_in[tensor].at[step])
            return total + wide(b_in[tensor].at[step]) + wide(a_in[tensor].at[step])

        for hop in (1, 2, 3):
            mine[tensor].at[hop][...] = total_of(hop).astype(mine[tensor].dtype)
            to_z(tensor, hop).start()
        mine_total = total_of(0)
        output_part(tensor)[...] = mine_total
    for tensor in range(count):
        out = output_part(tensor)
        total = out[...]
        for hop in (1, 2, 3):
            slot = PLANES - hop - 1
            pltpu.make_async_remote_copy(
                src_ref=mine[tensor].at[hop],
                dst_ref=z_in[tensor].at[slot],
                send_sem=z_send.at[tensor, hop - 1],
                recv_sem=z_recv.at[tensor, slot],
                device_id=sibling,
                device_id_type=MESH,
            ).wait_recv()
            total += wide(z_in[tensor].at[slot])
        out[...] = total
        to_output(tensor).start()
    for tensor in range(count):
        pltpu.make_async_remote_copy(
            src_ref=part_of(totals[tensor], splits[tensor], 0, 1 - half, 1, 8),
            dst_ref=part_of(totals[tensor], splits[tensor], 0, 1 - half, 1, 8),
            send_sem=o_send.at[tensor],
            recv_sem=o_recv.at[tensor],
            device_id=sibling,
            device_id_type=MESH,
        ).wait_recv()
        to_output(tensor).wait_send()
        for step, first, second in order:
            to_core(tensor, step, first, second).wait_send()
            if second == 1:
                to_b(tensor, step, first).wait_send()
            elif first == 1:
                to_a(tensor, step).wait_send()
            elif step > 0:
                to_z(tensor, step).wait_send()


def reduce_all(partials, splits, owners, collective_id):
    count = len(partials)
    aligns = [16 if part.dtype == jnp.bfloat16 else 8 for part in partials]
    dma = pltpu.SemaphoreType.DMA

    def pieces(slots):
        shapes = []
        for part, split in zip(partials, splits):
            rows, columns = part.shape[0] // owners, part.shape[1]
            shape = (rows, columns // 2) if split == COLUMN_SPLIT else (rows // 2, columns)
            shapes.append(pltpu.VMEM((slots, *shape), part.dtype))
        return shapes

    return pl.pallas_call(
        functools.partial(reduce_kernel, splits, aligns, owners),
        out_shape=[
            jax.ShapeDtypeStruct((part.shape[0] // owners, part.shape[1]), jnp.float32)
            for part in partials
        ],
        in_specs=[pl.BlockSpec(memory_space=pl.ANY)] * count,
        out_specs=[pl.BlockSpec(memory_space=pltpu.VMEM)] * count,
        scratch_shapes=[
            *pieces(16),
            *pieces(16),
            *pieces(8),
            *pieces(4),
            *pieces(3),
            dma((count, 16)),
            dma((count, 16)),
            dma((count, 16)),
            dma((count, 8)),
            dma((count, 8)),
            dma((count, 4)),
            dma((count, 4)),
            dma((count, 3)),
            dma((count, 3)),
            dma((count,)),
            dma((count,)),
        ],
        compiler_params=pltpu.CompilerParams(
            collective_id=collective_id, has_side_effects=True, vmem_limit_bytes=48 * 1024 * 1024
        ),
        name="reduce_rows",
    )(*partials)


OWNERS = 16
VECTOR_ROWS = 16
WEIGHT_SPLITS = (COLUMN_SPLIT, COLUMN_SPLIT, ROW_SPLIT, ROW_SPLIT)


def pack_vectors(parts, owners):
    grid = jnp.concatenate([p.astype(jnp.float32).reshape(owners, -1) for p in parts], axis=1)
    grid = jnp.pad(grid, ((0, 0), (0, VECTOR_ROWS * 128 - grid.shape[1])))
    return grid.reshape(owners * VECTOR_ROWS, 128)


def unpack_vectors(rows, owners, sizes):
    grid = rows.reshape(owners, VECTOR_ROWS * 128)
    vectors, start = [], 0
    for size in sizes:
        vectors.append(grid[:, start : start + size].reshape(owners * size))
        start += size
    return vectors


def gather_weights(matrices, vectors, use_kernels):
    if not use_kernels:
        whole = [lax.all_gather(m, "fsdp", axis=0, tiled=True) for m in (*matrices, *vectors)]
        return whole[: len(matrices)], whole[len(matrices) :]
    square = jnp.concatenate(matrices[:4], axis=1)
    packed = pack_vectors(vectors, 1)
    square, inner, outer, packed = gather_all(
        (square, matrices[4], matrices[5], packed), WEIGHT_SPLITS, OWNERS, 1
    )
    whole_vectors = unpack_vectors(packed, OWNERS, [v.shape[0] for v in vectors])
    return [*jnp.split(square, 4, axis=1), inner, outer], whole_vectors


def reduce_weights(matrices, vectors, use_kernels):
    if not use_kernels:
        totals = []
        for part in (*matrices, *vectors):
            share = lax.psum_scatter(part, "fsdp", scatter_dimension=0, tiled=True)
            totals.append(lax.psum(share.astype(jnp.bfloat16), "rep").astype(jnp.float32))
        return totals[: len(matrices)], totals[len(matrices) :]
    low = [m.astype(jnp.bfloat16) for m in matrices]
    square = jnp.concatenate(low[:4], axis=1)
    packed = pack_vectors(vectors, OWNERS)
    square, inner, outer, packed = reduce_all(
        (square, low[4], low[5], packed), WEIGHT_SPLITS, OWNERS, 2
    )
    sizes = [v.shape[0] // OWNERS for v in vectors]
    return [*jnp.split(square, 4, axis=1), inner, outer], unpack_vectors(packed, 1, sizes)


def on_device(
    use_kernels,
    captions,
    regions,
    caption_lengths,
    region_counts,
    group_ids,
    query_weight,
    key_weight,
    value_weight,
    out_weight,
    query_bias,
    value_bias,
    out_bias,
    first_gain,
    first_shift,
    inner_weight,
    inner_bias,
    outer_weight,
    outer_bias,
    second_gain,
    second_shift,
    caption_cotangent,
    region_cotangent,
):
    seq_count = captions.shape[0]
    caption_slots = captions.shape[1]
    width_model = captions.shape[2]
    image_count = regions.shape[0]
    region_slots = regions.shape[1]
    row_length = caption_slots + region_slots
    head_count = HEADS
    head_size = width_model // head_count
    scaling = head_size ** (-0.5)
    all_rows = seq_count * row_length
    (query_all, key_all, value_all, out_all, inner_all, outer_all), whole_vectors = gather_weights(
        (query_weight, key_weight, value_weight, out_weight, inner_weight, outer_weight),
        (
            query_bias,
            value_bias,
            out_bias,
            first_gain,
            first_shift,
            inner_bias,
            outer_bias,
            second_gain,
            second_shift,
        ),
        use_kernels,
    )
    (
        query_offset,
        value_offset,
        out_offset,
        gain_first,
        shift_first,
        inner_offset,
        outer_offset,
        gain_second,
        shift_second,
    ) = whole_vectors
    image_match = group_ids[:, None] == jnp.arange(image_count, dtype=jnp.int32)[None, :]
    match_low = image_match.astype(jnp.bfloat16)
    match_float = image_match.astype(jnp.float32)
    seq_regions = jnp.sum(jnp.where(image_match, region_counts[None, :], 0), axis=1)
    caption_live = jnp.arange(caption_slots, dtype=jnp.int32)[None, :] < caption_lengths[:, None]
    region_live = jnp.arange(region_slots, dtype=jnp.int32)[None, :] < seq_regions[:, None]
    live_rows = jnp.concatenate([caption_live, region_live], axis=1)
    live_column = live_rows.reshape(all_rows, 1).astype(jnp.float32)

    def spread_images(table):
        spread_out = jnp.einsum("si,ird->srd", match_low, table, preferred_element_type=jnp.float32)
        return spread_out.astype(jnp.bfloat16)

    def collect_images(gradient):
        summed = jnp.einsum("si,srd->ird", match_float, gradient, precision=HIGHEST_PRECISION)
        return summed.reshape(image_count * region_slots, width_model)

    caption_flat = captions.reshape(seq_count * caption_slots, width_model)
    region_flat = regions.reshape(image_count * region_slots, width_model)

    def sequence_rows(caption_part, image_part):
        caption_block = caption_part.reshape(seq_count, caption_slots, width_model)
        image_block = spread_images(image_part.reshape(image_count, region_slots, width_model))
        joined = jnp.concatenate([caption_block, image_block], axis=1)
        return joined.reshape(seq_count, row_length, head_count, head_size)

    def project_three(row_block):
        query_rows = (forward_rows(row_block, query_all) + query_offset.astype(jnp.float32)).astype(
            jnp.bfloat16
        )
        key_rows = forward_rows(row_block, key_all).astype(jnp.bfloat16)
        value_rows = (forward_rows(row_block, value_all) + value_offset.astype(jnp.float32)).astype(
            jnp.bfloat16
        )
        return (query_rows, key_rows, value_rows)

    query_caption, key_caption, value_caption = project_three(caption_flat)
    query_image, key_image, value_image = project_three(region_flat)
    queries = sequence_rows(query_caption, query_image)
    keys_seq = sequence_rows(key_caption, key_image)
    values_seq = sequence_rows(value_caption, value_image)

    def masked_scores():
        products = (
            jnp.einsum("sqhe,skhe->shqk", queries, keys_seq, preferred_element_type=jnp.float32)
            * scaling
        )
        return jnp.where(live_rows[:, None, None, :], products, MASKED_SCORE)

    scores = masked_scores()
    row_max = jnp.max(scores, axis=-1, keepdims=True)
    log_total = row_max + jnp.log(jnp.sum(jnp.exp(scores - row_max), axis=-1, keepdims=True))
    probs_low = jnp.exp(scores - log_total).astype(jnp.bfloat16)
    context = jnp.einsum(
        "shqk,skhe->sqhe", probs_low, values_seq, preferred_element_type=jnp.float32
    )
    context = context.astype(jnp.bfloat16).reshape(all_rows, width_model)
    inputs_seq = jnp.concatenate([captions, spread_images(regions)], axis=1).reshape(
        all_rows, width_model
    )
    first_sum = (
        inputs_seq.astype(jnp.float32)
        + forward_rows(context, out_all)
        + out_offset.astype(jnp.float32)
    )
    first_out, first_back = jax.vjp(
        normalize, first_sum, gain_first.astype(jnp.float32), shift_first.astype(jnp.float32)
    )
    first_low = first_out.astype(jnp.bfloat16)
    inner_pre = forward_rows(first_low, inner_all) + inner_offset.astype(jnp.float32)
    active_low = exact_gelu(inner_pre).astype(jnp.bfloat16)
    second_sum = first_out + forward_rows(active_low, outer_all) + outer_offset.astype(jnp.float32)
    second_out, second_back = jax.vjp(
        normalize, second_sum, gain_second.astype(jnp.float32), shift_second.astype(jnp.float32)
    )
    layer_out = (second_out * live_column).reshape(seq_count, row_length, width_model)
    out_caption = layer_out[:, :caption_slots].astype(jnp.bfloat16)
    out_region = layer_out[:, caption_slots:].astype(jnp.bfloat16)
    cotangent = jnp.concatenate([caption_cotangent, region_cotangent], axis=1)
    cotangent = cotangent.reshape(all_rows, width_model).astype(jnp.float32) * live_column
    second_grad, second_gain_grad, second_shift_grad = second_back(cotangent)
    inner_back, outer_back = (inner_all, outer_all)
    outer_grad = second_grad.astype(jnp.bfloat16)
    outer_weight_grad = weight_grad(active_low, outer_grad)
    outer_bias_grad = column_sum(outer_grad)
    active_grad = backward_rows(outer_grad, outer_back)
    inner_grad = jax.vjp(exact_gelu, inner_pre)[1](active_grad)[0].astype(jnp.bfloat16)
    inner_weight_grad = weight_grad(first_low, inner_grad)
    inner_bias_grad = column_sum(inner_grad)
    first_grad = second_grad + backward_rows(inner_grad, inner_back)
    sum_grad, first_gain_grad, first_shift_grad = first_back(first_grad)
    query_back, key_back, value_back, out_back = (query_all, key_all, value_all, out_all)
    attended_grad = sum_grad.astype(jnp.bfloat16)
    out_weight_grad = weight_grad(context, attended_grad)
    out_bias_grad = column_sum(attended_grad)
    context_grad = backward_rows(attended_grad, out_back).astype(jnp.bfloat16)
    context_grad = context_grad.reshape(seq_count, row_length, head_count, head_size)
    scores_again = masked_scores()
    probs_again = jnp.exp(scores_again - log_total)
    probs_grad = jnp.einsum(
        "sqhe,skhe->shqk", context_grad, values_seq, preferred_element_type=jnp.float32
    )
    value_grad = jnp.einsum(
        "shqk,sqhe->skhe",
        probs_again.astype(jnp.bfloat16),
        context_grad,
        preferred_element_type=jnp.float32,
    )
    row_inner = jnp.sum(probs_grad * probs_again, axis=-1, keepdims=True)
    score_grad = (probs_again * (probs_grad - row_inner)).astype(jnp.bfloat16)
    query_grad = (
        jnp.einsum("shqk,skhe->sqhe", score_grad, keys_seq, preferred_element_type=jnp.float32)
        * scaling
    )
    key_grad = (
        jnp.einsum("shqk,sqhe->skhe", score_grad, queries, preferred_element_type=jnp.float32)
        * scaling
    )

    def split_grad(gradient):
        grid = gradient.reshape(seq_count, row_length, width_model)
        caption_part = grid[:, :caption_slots].reshape(seq_count * caption_slots, width_model)
        image_part = collect_images(grid[:, caption_slots:])
        return (caption_part.astype(jnp.bfloat16), image_part.astype(jnp.bfloat16))

    query_cap_grad, query_img_grad = split_grad(query_grad)
    key_cap_grad, key_img_grad = split_grad(key_grad)
    value_cap_grad, value_img_grad = split_grad(value_grad)
    query_weight_grad = weight_grad(caption_flat, query_cap_grad) + weight_grad(
        region_flat, query_img_grad
    )
    query_bias_grad = column_sum(query_cap_grad) + column_sum(query_img_grad)
    key_weight_grad = weight_grad(caption_flat, key_cap_grad) + weight_grad(
        region_flat, key_img_grad
    )
    value_weight_grad = weight_grad(caption_flat, value_cap_grad) + weight_grad(
        region_flat, value_img_grad
    )
    value_bias_grad = column_sum(value_cap_grad) + column_sum(value_img_grad)
    sum_grid = sum_grad.reshape(seq_count, row_length, width_model)
    caption_input = sum_grid[:, :caption_slots].reshape(seq_count * caption_slots, width_model)
    caption_input = (
        caption_input
        + backward_rows(query_cap_grad, query_back)
        + backward_rows(key_cap_grad, key_back)
        + backward_rows(value_cap_grad, value_back)
    )
    grad_captions = caption_input.reshape(seq_count, caption_slots, width_model)
    region_input = (
        collect_images(sum_grid[:, caption_slots:])
        + backward_rows(query_img_grad, query_back)
        + backward_rows(key_img_grad, key_back)
        + backward_rows(value_img_grad, value_back)
    )
    grad_regions = region_input.reshape(image_count, region_slots, width_model)
    matrix_totals, vector_totals = reduce_weights(
        (
            query_weight_grad,
            key_weight_grad,
            value_weight_grad,
            out_weight_grad,
            inner_weight_grad,
            outer_weight_grad,
        ),
        (
            query_bias_grad,
            value_bias_grad,
            out_bias_grad,
            first_gain_grad,
            first_shift_grad,
            inner_bias_grad,
            outer_bias_grad,
            second_gain_grad,
            second_shift_grad,
        ),
        use_kernels,
    )
    query_total, key_total, value_total, out_total, inner_total, outer_total = matrix_totals
    return (
        out_caption,
        out_region,
        grad_captions,
        grad_regions,
        query_total,
        key_total,
        value_total,
        out_total,
        *vector_totals[:5],
        inner_total,
        vector_totals[5],
        outer_total,
        *vector_totals[6:],
    )


def solution(mesh):
    use_kernels = mesh.shape["fsdp"] == OWNERS
    return jax.shard_map(
        functools.partial(on_device, use_kernels),
        mesh=mesh,
        in_specs=(
            P(("fsdp", "rep"), None, None),
            P(("fsdp", "rep"), None, None),
            P(("fsdp", "rep")),
            P(("fsdp", "rep")),
            P(("fsdp", "rep")),
            P("fsdp", None),
            P("fsdp", None),
            P("fsdp", None),
            P("fsdp", None),
            P("fsdp"),
            P("fsdp"),
            P("fsdp"),
            P("fsdp"),
            P("fsdp"),
            P("fsdp", None),
            P("fsdp"),
            P("fsdp", None),
            P("fsdp"),
            P("fsdp"),
            P("fsdp"),
            P(("fsdp", "rep"), None, None),
            P(("fsdp", "rep"), None, None),
        ),
        out_specs=(
            P(("fsdp", "rep"), None, None),
            P(("fsdp", "rep"), None, None),
            P(("fsdp", "rep"), None, None),
            P(("fsdp", "rep"), None, None),
            P("fsdp", None),
            P("fsdp", None),
            P("fsdp", None),
            P("fsdp", None),
            P("fsdp"),
            P("fsdp"),
            P("fsdp"),
            P("fsdp"),
            P("fsdp"),
            P("fsdp", None),
            P("fsdp"),
            P("fsdp", None),
            P("fsdp"),
            P("fsdp"),
            P("fsdp"),
        ),
        check_vma=False,
    )
```

```python
import functools

import jax
import jax.numpy as jnp
from jax import lax
from jax.experimental import pallas as pl
from jax.experimental.pallas import tpu as pltpu
from jax.sharding import PartitionSpec as P

EPSILON = 1e-12
MASKED_SCORE = -1e30

MESH = pl.DeviceIdType.MESH
PLANES = 4
COLUMN_SPLIT, ROW_SPLIT = 0, 1


def place_of(index, half, step, first, second):
    across = first * (1 - half) + second * half
    down = second * (1 - half) + first * half
    plane = lax.rem(index // 4 + step, PLANES)
    row = lax.rem(lax.rem(index // 2, 2) + down, 2)
    column = lax.rem(lax.rem(index, 2) + across, 2)
    return plane * 4 + row * 2 + column


def part_of(ref, split, owner, half, count, align):
    rows, columns = ref.shape[0] // count, ref.shape[1]
    if split == COLUMN_SPLIT:
        width = columns // 2
        return ref.at[
            pl.ds(pl.multiple_of(owner * rows, align), rows),
            pl.ds(pl.multiple_of(half * width, 128), width),
        ]
    height = rows // 2
    return ref.at[pl.ds(pl.multiple_of(owner * rows + half * height, align), height)]


def greet(index, half):
    barrier = pltpu.get_barrier_semaphore()
    peers = [(place_of(index, half, step, 0, 0), half) for step in (1, 2, 3)]
    peers += [(place_of(index, half, 0, 1, 0), half), (place_of(index, half, 0, 0, 1), half)]
    peers += [(index, 1 - half)]
    for peer in peers:
        pl.semaphore_signal(barrier, inc=1, device_id=peer, device_id_type=MESH)
    pl.semaphore_wait(barrier, len(peers))


def gather_kernel(splits, aligns, *refs):
    count = len(splits)
    shards, wholes = refs[:count], refs[count : 2 * count]
    (own_sem, z_send, z_recv, a_send, a_recv, b_send, b_recv, s_send, s_recv) = refs[2 * count :]
    index, half = lax.axis_index("fsdp"), lax.axis_index("rep")
    owners = wholes[0].shape[0] // shards[0].shape[0]

    def owner_of(step, first, second):
        return place_of(index, half, step, first, second)

    def piece(tensor, step, first, second):
        owner = owner_of(step, first, second)
        return part_of(wholes[tensor], splits[tensor], owner, half, owners, aligns[tensor])

    def copy_piece(tensor, source, step, first, second, send, recv, peer):
        return pltpu.make_async_remote_copy(
            src_ref=source,
            dst_ref=piece(tensor, step, first, second),
            send_sem=send,
            recv_sem=recv,
            device_id=peer,
            device_id_type=MESH,
        )

    peer_a = (owner_of(0, 1, 0), half)
    peer_b = (owner_of(0, 0, 1), half)
    sibling = (index, 1 - half)

    def to_z(tensor, source, hop):
        peer = (owner_of(hop, 0, 0), half)
        slot = PLANES - hop - 1
        return copy_piece(
            tensor, source, 0, 0, 0, z_send.at[tensor, hop - 1], z_recv.at[tensor, slot], peer
        )

    def to_a(tensor, source, step):
        return copy_piece(
            tensor, source, step, 0, 0, a_send.at[tensor, step], a_recv.at[tensor, step], peer_a
        )

    def to_b(tensor, source, step, first):
        slot = step * 2 + first
        return copy_piece(
            tensor, source, step, first, 0, b_send.at[tensor, slot], b_recv.at[tensor, slot], peer_b
        )

    def to_sibling(tensor, source, step, first, second):
        slot = step * 4 + first * 2 + second - 1
        return copy_piece(
            tensor,
            source,
            step,
            first,
            second,
            s_send.at[tensor, slot],
            s_recv.at[tensor, slot],
            sibling,
        )

    greet(index, half)
    started = []
    local = []
    for tensor in range(count):
        shard = shards[tensor]
        rows = shard.shape[0]
        source = part_of(shard, splits[tensor], 0, half, 1, aligns[tensor])
        sends = [to_z(tensor, source, hop) for hop in (1, 2, 3)]
        sends += [to_a(tensor, source, 0), to_b(tensor, source, 0, 0)]
        for copy in sends:
            copy.start()
        started += sends
        here = pltpu.make_async_copy(
            shard,
            wholes[tensor].at[pl.ds(pl.multiple_of(index * rows, aligns[tensor]), rows)],
            own_sem.at[tensor],
        )
        here.start()
        local.append(here)
    for tensor in range(count):
        for step in (1, 2, 3):
            source = piece(tensor, step, 0, 0)
            copy_piece(
                tensor,
                source,
                step,
                0,
                0,
                z_send.at[tensor, step - 1],
                z_recv.at[tensor, step - 1],
                sibling,
            ).wait_recv()
            sends = [
                to_b(tensor, source, step, 0),
                to_a(tensor, source, step),
                to_sibling(tensor, source, step, 0, 0),
            ]
            for copy in sends:
                copy.start()
            started += sends
    for tensor in range(count):
        for step in range(PLANES):
            source = piece(tensor, step, 1, 0)
            copy_piece(
                tensor,
                source,
                step,
                1,
                0,
                a_send.at[tensor, step],
                a_recv.at[tensor, step],
                peer_a,
            ).wait_recv()
            sends = [to_b(tensor, source, step, 1), to_sibling(tensor, source, step, 1, 0)]
            for copy in sends:
                copy.start()
            started += sends
    for tensor in range(count):
        for step in range(PLANES):
            for first in (0, 1):
                source = piece(tensor, step, first, 1)
                slot = step * 2 + first
                copy_piece(
                    tensor,
                    source,
                    step,
                    first,
                    1,
                    b_send.at[tensor, slot],
                    b_recv.at[tensor, slot],
                    peer_b,
                ).wait_recv()
                copy = to_sibling(tensor, source, step, first, 1)
                copy.start()
                started.append(copy)
    for tensor in range(count):
        local[tensor].wait()
        for step in range(PLANES):
            for first in (0, 1):
                for second in (0, 1):
                    if step + first + second == 0:
                        continue
                    slot = step * 4 + first * 2 + second - 1
                    owner = place_of(index, 1 - half, step, first, second)
                    there = part_of(
                        wholes[tensor], splits[tensor], owner, 1 - half, owners, aligns[tensor]
                    )
                    pltpu.make_async_remote_copy(
                        src_ref=there,
                        dst_ref=there,
                        send_sem=s_send.at[tensor, slot],
                        recv_sem=s_recv.at[tensor, slot],
                        device_id=sibling,
                        device_id_type=MESH,
                    ).wait_recv()
    for copy in started:
        copy.wait_send()


def gather_all(shards, splits, owners, collective_id):
    count = len(shards)
    aligns = [16 if shard.dtype == jnp.bfloat16 else 8 for shard in shards]
    dma = pltpu.SemaphoreType.DMA
    return pl.pallas_call(
        functools.partial(gather_kernel, splits, aligns),
        out_shape=[
            jax.ShapeDtypeStruct((owners * shard.shape[0], shard.shape[1]), shard.dtype)
            for shard in shards
        ],
        in_specs=[pl.BlockSpec(memory_space=pltpu.VMEM)] * count,
        out_specs=[pl.BlockSpec(memory_space=pl.ANY)] * count,
        scratch_shapes=[
            dma((count,)),
            dma((count, 3)),
            dma((count, 3)),
            dma((count, 4)),
            dma((count, 4)),
            dma((count, 8)),
            dma((count, 8)),
            dma((count, 15)),
            dma((count, 15)),
        ],
        compiler_params=pltpu.CompilerParams(collective_id=collective_id, has_side_effects=True),
        name="gather_rows",
    )(*shards)


def reduce_kernel(splits, aligns, owners, *refs):
    count = len(splits)
    partials, totals = refs[:count], refs[count : 2 * count]
    mine = refs[2 * count : 3 * count]
    core_in = refs[3 * count : 4 * count]
    b_in = refs[4 * count : 5 * count]
    a_in = refs[5 * count : 6 * count]
    z_in = refs[6 * count : 7 * count]
    (load_sem, c_send, c_recv, b_send, b_recv, a_send, a_recv, z_send, z_recv, o_send, o_recv) = (
        refs[7 * count :]
    )
    index, half = lax.axis_index("fsdp"), lax.axis_index("rep")
    sibling = (index, 1 - half)
    peer_a = (place_of(index, half, 0, 1, 0), half)
    peer_b = (place_of(index, half, 0, 0, 1), half)

    def slot_of(step, first, second):
        return second * 8 + first * 4 + step

    def load(tensor, step, first, second):
        owner = place_of(index, half, step, first, second)
        slot = slot_of(step, first, second)
        return pltpu.make_async_copy(
            part_of(partials[tensor], splits[tensor], owner, half, owners, aligns[tensor]),
            mine[tensor].at[slot],
            load_sem.at[tensor, slot],
        )

    def to_core(tensor, step, first, second):
        owner = place_of(index, 1 - half, step, first, second)
        slot = slot_of(step, first, second)
        return pltpu.make_async_remote_copy(
            src_ref=part_of(
                partials[tensor], splits[tensor], owner, 1 - half, owners, aligns[tensor]
            ),
            dst_ref=core_in[tensor].at[slot],
            send_sem=c_send.at[tensor, slot],
            recv_sem=c_recv.at[tensor, slot],
            device_id=sibling,
            device_id_type=MESH,
        )

    def to_b(tensor, step, first):
        slot = first * 4 + step
        return pltpu.make_async_remote_copy(
            src_ref=mine[tensor].at[8 + slot],
            dst_ref=b_in[tensor].at[slot],
            send_sem=b_send.at[tensor, slot],
            recv_sem=b_recv.at[tensor, slot],
            device_id=peer_b,
            device_id_type=MESH,
        )

    def to_a(tensor, step):
        return pltpu.make_async_remote_copy(
            src_ref=mine[tensor].at[4 + step],
            dst_ref=a_in[tensor].at[step],
            send_sem=a_send.at[tensor, step],
            recv_sem=a_recv.at[tensor, step],
            device_id=peer_a,
            device_id_type=MESH,
        )

    def to_z(tensor, hop):
        return pltpu.make_async_remote_copy(
            src_ref=mine[tensor].at[hop],
            dst_ref=z_in[tensor].at[PLANES - hop - 1],
            send_sem=z_send.at[tensor, hop - 1],
            recv_sem=z_recv.at[tensor, PLANES - hop - 1],
            device_id=(place_of(index, half, hop, 0, 0), half),
            device_id_type=MESH,
        )

    def wide(ref):
        return ref[...].astype(jnp.float32)

    def output_part(tensor):
        return part_of(totals[tensor], splits[tensor], 0, half, 1, 8)

    def to_output(tensor):
        return pltpu.make_async_remote_copy(
            src_ref=output_part(tensor),
            dst_ref=output_part(tensor),
            send_sem=o_send.at[tensor],
            recv_sem=o_recv.at[tensor],
            device_id=sibling,
            device_id_type=MESH,
        )

    greet(index, half)

    order = [(step, first, 1) for first in (1, 0) for step in (1, 2, 3, 0)]
    order += [(step, 1, 0) for step in (1, 2, 3, 0)] + [(step, 0, 0) for step in (1, 2, 3, 0)]
    for tensor in range(count):
        for step, first, second in order:
            to_core(tensor, step, first, second).start()
            load(tensor, step, first, second).start()

    for tensor in range(count):

        def b_step(turn, carry, tensor=tensor):
            step, first = lax.rem(turn + 1, PLANES), 1 - turn // PLANES
            load(tensor, step, first, 1).wait()
            to_core(tensor, step, first, 1).wait_recv()
            slot = slot_of(step, first, 1)
            total = wide(mine[tensor].at[slot]) + wide(core_in[tensor].at[slot])
            mine[tensor].at[slot][...] = total.astype(mine[tensor].dtype)
            to_b(tensor, step, first).start()
            return carry

        lax.fori_loop(0, 2 * PLANES, b_step, 0)
    for tensor in range(count):

        def a_step(turn, carry, tensor=tensor):
            step = lax.rem(turn + 1, PLANES)
            load(tensor, step, 1, 0).wait()
            to_core(tensor, step, 1, 0).wait_recv()
            to_b(tensor, step, 1).wait_recv()
            slot = slot_of(step, 1, 0)
            total = wide(mine[tensor].at[slot]) + wide(core_in[tensor].at[slot])
            total += wide(b_in[tensor].at[slot])
            mine[tensor].at[slot][...] = total.astype(mine[tensor].dtype)
            to_a(tensor, step).start()
            return carry

        lax.fori_loop(0, PLANES, a_step, 0)
    for tensor in range(count):

        def total_of(step, tensor=tensor):
            load(tensor, step, 0, 0).wait()
            to_core(tensor, step, 0, 0).wait_recv()
            to_b(tensor, step, 0).wait_recv()
            to_a(tensor, step).wait_recv()
            total = wide(mine[tensor].at[step]) + wide(core_in[tensor].at[step])
            return total + wide(b_in[tensor].at[step]) + wide(a_in[tensor].at[step])

        for hop in (1, 2, 3):
            mine[tensor].at[hop][...] = total_of(hop).astype(mine[tensor].dtype)
            to_z(tensor, hop).start()
        mine_total = total_of(0)
        output_part(tensor)[...] = mine_total
    for tensor in range(count):
        out = output_part(tensor)
        total = out[...]
        for hop in (1, 2, 3):
            slot = PLANES - hop - 1
            pltpu.make_async_remote_copy(
                src_ref=mine[tensor].at[hop],
                dst_ref=z_in[tensor].at[slot],
                send_sem=z_send.at[tensor, hop - 1],
                recv_sem=z_recv.at[tensor, slot],
                device_id=sibling,
                device_id_type=MESH,
            ).wait_recv()
            total += wide(z_in[tensor].at[slot])
        out[...] = total
        to_output(tensor).start()
    for tensor in range(count):
        pltpu.make_async_remote_copy(
            src_ref=part_of(totals[tensor], splits[tensor], 0, 1 - half, 1, 8),
            dst_ref=part_of(totals[tensor], splits[tensor], 0, 1 - half, 1, 8),
            send_sem=o_send.at[tensor],
            recv_sem=o_recv.at[tensor],
            device_id=sibling,
            device_id_type=MESH,
        ).wait_recv()
        to_output(tensor).wait_send()
        for step, first, second in order:
            to_core(tensor, step, first, second).wait_send()
            if second == 1:
                to_b(tensor, step, first).wait_send()
            elif first == 1:
                to_a(tensor, step).wait_send()
            elif step > 0:
                to_z(tensor, step).wait_send()


def reduce_all(partials, splits, owners, collective_id):
    count = len(partials)
    aligns = [16 if part.dtype == jnp.bfloat16 else 8 for part in partials]
    dma = pltpu.SemaphoreType.DMA

    def pieces(slots):
        shapes = []
        for part, split in zip(partials, splits):
            rows, columns = part.shape[0] // owners, part.shape[1]
            shape = (rows, columns // 2) if split == COLUMN_SPLIT else (rows // 2, columns)
            shapes.append(pltpu.VMEM((slots, *shape), part.dtype))
        return shapes

    return pl.pallas_call(
        functools.partial(reduce_kernel, splits, aligns, owners),
        out_shape=[
            jax.ShapeDtypeStruct((part.shape[0] // owners, part.shape[1]), jnp.float32)
            for part in partials
        ],
        in_specs=[pl.BlockSpec(memory_space=pl.ANY)] * count,
        out_specs=[pl.BlockSpec(memory_space=pltpu.VMEM)] * count,
        scratch_shapes=[
            *pieces(16),
            *pieces(16),
            *pieces(8),
            *pieces(4),
            *pieces(3),
            dma((count, 16)),
            dma((count, 16)),
            dma((count, 16)),
            dma((count, 8)),
            dma((count, 8)),
            dma((count, 4)),
            dma((count, 4)),
            dma((count, 3)),
            dma((count, 3)),
            dma((count,)),
            dma((count,)),
        ],
        compiler_params=pltpu.CompilerParams(
            collective_id=collective_id, has_side_effects=True, vmem_limit_bytes=48 * 1024 * 1024
        ),
        name="reduce_rows",
    )(*partials)


OWNERS = 16
VECTOR_ROWS = 16
WEIGHT_SPLITS = (COLUMN_SPLIT, COLUMN_SPLIT, ROW_SPLIT, ROW_SPLIT)


def pack_vectors(parts, owners):
    grid = jnp.concatenate([p.astype(jnp.float32).reshape(owners, -1) for p in parts], axis=1)
    grid = jnp.pad(grid, ((0, 0), (0, VECTOR_ROWS * 128 - grid.shape[1])))
    return grid.reshape(owners * VECTOR_ROWS, 128)


def unpack_vectors(rows, owners, sizes):
    grid = rows.reshape(owners, VECTOR_ROWS * 128)
    vectors, start = [], 0
    for size in sizes:
        vectors.append(grid[:, start : start + size].reshape(owners * size))
        start += size
    return vectors


def gather_weights(squares, inner, outer, vectors, use_kernels):
    square = jnp.concatenate(squares, axis=1)
    if not use_kernels:
        whole = [lax.all_gather(m, "fsdp", axis=0, tiled=True) for m in (square, inner, outer)]
        return *whole, [lax.all_gather(v, "fsdp", axis=0, tiled=True) for v in vectors]
    packed = pack_vectors(vectors, 1)
    square, inner, outer, packed = gather_all(
        (square, inner, outer, packed), WEIGHT_SPLITS, OWNERS, 1
    )
    return square, inner, outer, unpack_vectors(packed, OWNERS, [v.shape[0] for v in vectors])


def reduce_weights(square, inner, outer, vectors, use_kernels):
    if not use_kernels:
        totals = []
        for part in (square, inner, outer, *vectors):
            wide = part.astype(jnp.float32)
            share = lax.psum_scatter(wide, "fsdp", scatter_dimension=0, tiled=True)
            totals.append(lax.psum(share.astype(jnp.bfloat16), "rep").astype(jnp.float32))
        return *totals[:3], totals[3:]
    packed = pack_vectors(vectors, OWNERS)
    square, inner, outer, packed = reduce_all(
        (square, inner, outer, packed), WEIGHT_SPLITS, OWNERS, 2
    )
    sizes = [v.shape[0] // OWNERS for v in vectors]
    return square, inner, outer, unpack_vectors(packed, 1, sizes)


def dot_nn(left, right):
    return lax.dot_general(
        left, right, (((1,), (0,)), ((), ())), preferred_element_type=jnp.float32
    )


def dot_nt(left, right):
    return lax.dot_general(
        left, right, (((1,), (1,)), ((), ())), preferred_element_type=jnp.float32
    )


def dot_tn(left, right):
    return lax.dot_general(
        left, right, (((0,), (0,)), ((), ())), preferred_element_type=jnp.float32
    )


HEAD = 64
EXTRA_ROWS = 16
HEADS_AT_ONCE = 2


def key_mask_rows(length, count, slots):
    slot = lax.broadcasted_iota(jnp.int32, (EXTRA_ROWS, 2 * slots), 1)
    row = lax.broadcasted_iota(jnp.int32, (EXTRA_ROWS, 2 * slots), 0)
    live = (slot < length) | ((slot >= slots) & (slot < slots + count))
    return jnp.where((row > 0) | live, 0.0, MASKED_SCORE).astype(jnp.bfloat16)


def query_mask_rows(slots):
    row = lax.broadcasted_iota(jnp.int32, (EXTRA_ROWS, 2 * slots), 0)
    return jnp.where(row == 0, 1.0, 0.0).astype(jnp.bfloat16)


def live_rows_column(length, count, slots):
    row = lax.broadcasted_iota(jnp.int32, (2 * slots, 1), 0)
    live = (row < length) | ((row >= slots) & (row < slots + count))
    return jnp.where(live, 1.0, 0.0)


def head_rows(cap_part, image_part, base):
    rows = pl.ds(pl.multiple_of(base, HEAD), HEAD)
    return jnp.concatenate([cap_part[rows, :], image_part[rows, :]], axis=1)


def project_kernel(length_ref, count_ref, group_ref, cap_ref, image_ref, weight_ref, bias_ref,
                   cap_out, image_out, context_out, lse_out, weight_turned, bias_wide):
    step = pl.program_id(0)
    width = cap_ref.shape[2]
    slots = cap_ref.shape[1]
    scaling = HEAD ** (-0.5)

    @pl.when(step == 0)
    def _():
        weight_turned[...] = weight_ref[:, : 3 * width].T
        bias_wide[...] = jnp.broadcast_to(bias_ref[...], (128, 3 * width)).T

    def project(rows):
        parts = []
        for part in range(3):
            turned = dot_nt(weight_turned[part * width : (part + 1) * width, :], rows)
            bias = bias_wide[part * width : (part + 1) * width, :]
            turned = turned + jnp.concatenate([bias, bias], axis=1)
            turned = turned.astype(jnp.bfloat16)
            parts.append(turned * scaling if part == 0 else turned)
        return parts

    @pl.when(step == 0)
    def _():
        parts = project(image_ref[...].reshape(2 * slots, width))
        for part in range(3):
            rows = slice(part * width, (part + 1) * width)
            image_out[0, rows, :] = parts[part][:, :slots]
            image_out[1, rows, :] = parts[part][:, slots:]

    @pl.when(lax.rem(step, 2) == 0)
    def _():
        parts = project(cap_ref[...].reshape(2 * slots, width))
        for part in range(3):
            rows = slice(part * width, (part + 1) * width)
            cap_out[0, rows, :] = parts[part][:, :slots]
            cap_out[1, rows, :] = parts[part][:, slots:]

    cap_part = cap_out.at[lax.rem(step, 2)]
    image_part = image_out.at[group_ref[step]]
    key_extra = key_mask_rows(length_ref[step], count_ref[step], slots)
    query_extra = query_mask_rows(slots)

    def heads(turn, carry):
        for inner in range(HEADS_AT_ONCE):
            head = turn * HEADS_AT_ONCE + inner
            query = head_rows(cap_part, image_part, head * HEAD)
            key = head_rows(cap_part, image_part, width + head * HEAD)
            value = head_rows(cap_part, image_part, 2 * width + head * HEAD)
            scores = dot_tn(
                jnp.concatenate([key, key_extra], axis=0),
                jnp.concatenate([query, query_extra], axis=0),
            )
            largest = jnp.max(scores, axis=0, keepdims=True)
            powers = jnp.exp(scores - largest)
            total = jnp.sum(powers, axis=0, keepdims=True)
            probs = (powers * (1.0 / total)).astype(jnp.bfloat16)
            context = dot_nn(value, probs)
            context_out[0, pl.ds(pl.multiple_of(head * HEAD, HEAD), HEAD), :] = context.astype(
                jnp.bfloat16
            )
            lse_out[0, pl.ds(head, 1), :] = largest + jnp.log(total)
        return carry

    lax.fori_loop(0, width // HEAD // HEADS_AT_ONCE, heads, 0)


def attend_forward(lengths, counts, groups, captions, regions, square, bias_row):
    seqs, slots, width = captions.shape
    images = regions.shape[0]
    heads = width // HEAD
    grid_spec = pltpu.PrefetchScalarGridSpec(
        num_scalar_prefetch=3,
        grid=(seqs,),
        in_specs=[
            pl.BlockSpec((2, slots, width), lambda s, *_: (s // 2, 0, 0)),
            pl.BlockSpec((images, slots, width), lambda s, *_: (0, 0, 0)),
            pl.BlockSpec(square.shape, lambda s, *_: (0, 0), pipeline_mode=pl.Buffered(1)),
            pl.BlockSpec(bias_row.shape, lambda s, *_: (0, 0)),
        ],
        out_specs=[
            pl.BlockSpec((2, 3 * width, slots), lambda s, *_: (s // 2, 0, 0)),
            pl.BlockSpec((images, 3 * width, slots), lambda s, *_: (0, 0, 0)),
            pl.BlockSpec((1, width, 2 * slots), lambda s, *_: (s, 0, 0)),
            pl.BlockSpec((1, heads, 2 * slots), lambda s, *_: (s, 0, 0)),
        ],
        scratch_shapes=[
            pltpu.VMEM((3 * width, width), jnp.bfloat16),
            pltpu.VMEM((3 * width, 128), jnp.float32),
        ],
    )
    return pl.pallas_call(
        project_kernel,
        grid_spec=grid_spec,
        out_shape=[
            jax.ShapeDtypeStruct((seqs, 3 * width, slots), jnp.bfloat16),
            jax.ShapeDtypeStruct((images, 3 * width, slots), jnp.bfloat16),
            jax.ShapeDtypeStruct((seqs, width, 2 * slots), jnp.bfloat16),
            jax.ShapeDtypeStruct((seqs, heads, 2 * slots), jnp.float32),
        ],
        compiler_params=pltpu.CompilerParams(vmem_limit_bytes=48 * 1024 * 1024),
        name="attend_forward",
    )(lengths, counts, groups, captions, regions, square, bias_row)


PHI_SLOPE = 0.2316419
PHI_TERMS = (0.319381530, -0.356563782, 1.781477937, -1.821255978, 1.330274429)
FF_CHUNK = 512


def gelu_both(values):
    density = 0.3989422804014327 * jnp.exp(-0.5 * values * values)
    ratio = 1.0 / (1.0 + PHI_SLOPE * jnp.abs(values))
    tail = PHI_TERMS[4]
    for term in PHI_TERMS[3::-1]:
        tail = tail * ratio + term
    tail = tail * ratio * density
    below = jnp.where(values >= 0.0, 1.0 - tail, tail)
    return values * below, below + values * density


def norm_parts(values):
    average = jnp.mean(values, axis=-1, keepdims=True)
    centred = values - average
    spread = jnp.mean(centred * centred, axis=-1, keepdims=True)
    inverse = lax.rsqrt(spread + EPSILON)
    return centred * inverse, inverse


def norm_back(gradient, gain, normal, inverse):
    scaled = gradient * gain
    first = jnp.mean(scaled, axis=-1, keepdims=True)
    second = jnp.mean(scaled * normal, axis=-1, keepdims=True)
    return (scaled - first - normal * second) * inverse


def feed_kernel(length_ref, count_ref, group_ref, context_ref, cap_ref, image_ref, cap_cot_ref,
                region_cot_ref, out_weight_ref, inner_ref, outer_ref, vector_ref, inner_bias_ref,
                out_cap_ref, out_region_ref, cap_sum_ref, region_sum_ref, context_grad_ref,
                out_grad_ref, inner_grad_ref, outer_grad_ref, vector_grad_ref, bias_grad_ref,
                active_sc, slope_sc, inner_acc, outer_acc, out_acc):
    step = pl.program_id(0)
    slots = cap_ref.shape[1]
    hidden = inner_ref.shape[1]
    chunks = [slice(start, start + FF_CHUNK) for start in range(0, hidden, FF_CHUNK)]

    @pl.when(step == 0)
    def _():
        inner_acc[...] = jnp.zeros_like(inner_acc)
        outer_acc[...] = jnp.zeros_like(outer_acc)
        out_acc[...] = jnp.zeros_like(out_acc)
        vector_grad_ref[...] = jnp.zeros_like(vector_grad_ref)
        bias_grad_ref[...] = jnp.zeros_like(bias_grad_ref)

    def vector(row):
        return vector_ref[row : row + 1, :]

    def add_vector(row, values):
        vector_grad_ref[row : row + 1, :] += jnp.sum(values, axis=0, keepdims=True)

    live = live_rows_column(length_ref[step], count_ref[step], slots)
    rows_in = jnp.concatenate([cap_ref[0], image_ref[0]], axis=0).astype(jnp.float32)
    first_sum = rows_in + dot_tn(context_ref[0], out_weight_ref[...]) + vector(0)
    first_normal, first_inverse = norm_parts(first_sum)
    first_out = first_normal * vector(1) + vector(2)
    first_low = first_out.astype(jnp.bfloat16)
    second_sum = first_out + vector(3)
    for chunk in chunks:
        pre = dot_nn(first_low, inner_ref[:, chunk]) + inner_bias_ref[:, chunk]
        active, slope = gelu_both(pre)
        active = active.astype(jnp.bfloat16)
        active_sc[:, chunk] = active
        slope_sc[:, chunk] = slope
        second_sum = second_sum + dot_nn(active, outer_ref[chunk, :])
    second_normal, second_inverse = norm_parts(second_sum)
    result = ((second_normal * vector(4) + vector(5)) * live).astype(jnp.bfloat16)
    out_cap_ref[0] = result[:slots]
    out_region_ref[0] = result[slots:]
    cot = jnp.concatenate([cap_cot_ref[0], region_cot_ref[0]], axis=0).astype(jnp.float32) * live
    add_vector(4, cot * second_normal)
    add_vector(5, cot)
    second_grad = norm_back(cot, vector(4), second_normal, second_inverse)
    outer_grad = second_grad.astype(jnp.bfloat16)
    add_vector(3, outer_grad.astype(jnp.float32))
    first_grad = second_grad
    first_turned = first_low.T
    for chunk in chunks:
        active_grad = dot_nt(outer_grad, outer_ref[chunk, :])
        inner_grad = (active_grad * slope_sc[:, chunk]).astype(jnp.bfloat16)
        bias_grad_ref[:, chunk] += jnp.sum(inner_grad.astype(jnp.float32), axis=0, keepdims=True)
        inner_acc[:, chunk] += dot_nn(first_turned, inner_grad)
        outer_acc[chunk, :] += dot_tn(active_sc[:, chunk], outer_grad)
        first_grad = first_grad + dot_nt(inner_grad, inner_ref[:, chunk])
    add_vector(1, first_grad * first_normal)
    add_vector(2, first_grad)
    sum_grad = norm_back(first_grad, vector(1), first_normal, first_inverse)
    cap_sum_ref[0] = sum_grad[:slots]
    region_sum_ref[0] = sum_grad[slots:]
    attended_grad = sum_grad.astype(jnp.bfloat16)
    add_vector(0, attended_grad.astype(jnp.float32))
    out_acc[...] += dot_nn(context_ref[0], attended_grad)
    context_grad_ref[0] = dot_nt(out_weight_ref[...], attended_grad).astype(jnp.bfloat16)

    @pl.when(step == pl.num_programs(0) - 1)
    def _():
        out_grad_ref[...] = out_acc[...].astype(jnp.bfloat16)
        inner_grad_ref[...] = inner_acc[...].astype(jnp.bfloat16)
        outer_grad_ref[...] = outer_acc[...].astype(jnp.bfloat16)


def feed_both(lengths, counts, groups, context, captions, regions, cap_cot, region_cot, square,
              inner, outer, vectors, inner_bias):
    seqs, slots, width = captions.shape
    hidden = inner.shape[1]
    once = pl.Buffered(1)

    def seq_block(*shape):
        return pl.BlockSpec((1, *shape), lambda s, *_: (s, 0, 0))

    def whole(shape, column=0):
        return pl.BlockSpec(shape, lambda s, *_: (0, column), pipeline_mode=once)

    grid_spec = pltpu.PrefetchScalarGridSpec(
        num_scalar_prefetch=3,
        grid=(seqs,),
        in_specs=[
            seq_block(width, 2 * slots),
            seq_block(slots, width),
            pl.BlockSpec((1, slots, width), lambda s, lens, counts, group: (group[s], 0, 0)),
            seq_block(slots, width),
            seq_block(slots, width),
            whole((width, width), 3),
            whole((width, hidden)),
            whole((hidden, width)),
            whole(vectors.shape),
            whole(inner_bias.shape),
        ],
        out_specs=[
            seq_block(slots, width),
            seq_block(slots, width),
            seq_block(slots, width),
            seq_block(slots, width),
            seq_block(width, 2 * slots),
            whole((width, width)),
            whole((width, hidden)),
            whole((hidden, width)),
            whole((8, width)),
            whole((1, hidden)),
        ],
        scratch_shapes=[
            pltpu.VMEM((2 * slots, hidden), jnp.bfloat16),
            pltpu.VMEM((2 * slots, hidden), jnp.float32),
            pltpu.VMEM((width, hidden), jnp.float32),
            pltpu.VMEM((hidden, width), jnp.float32),
            pltpu.VMEM((width, width), jnp.float32),
        ],
    )
    low, wide = jnp.bfloat16, jnp.float32
    rows_shape = (seqs, slots, width)
    return pl.pallas_call(
        feed_kernel,
        grid_spec=grid_spec,
        out_shape=[
            jax.ShapeDtypeStruct(rows_shape, low),
            jax.ShapeDtypeStruct(rows_shape, low),
            jax.ShapeDtypeStruct(rows_shape, wide),
            jax.ShapeDtypeStruct(rows_shape, wide),
            jax.ShapeDtypeStruct((seqs, width, 2 * slots), low),
            jax.ShapeDtypeStruct((width, width), low),
            jax.ShapeDtypeStruct((width, hidden), low),
            jax.ShapeDtypeStruct((hidden, width), low),
            jax.ShapeDtypeStruct((8, width), wide),
            jax.ShapeDtypeStruct((1, hidden), wide),
        ],
        compiler_params=pltpu.CompilerParams(vmem_limit_bytes=63 * 1024 * 1024),
        name="feed_both",
    )(lengths, counts, groups, context, captions, regions, cap_cot, region_cot, square, inner,
      outer, vectors, inner_bias)


def attend_back_kernel(length_ref, count_ref, group_ref, cap_ref, image_ref, lse_ref,
                       context_grad_ref, rows_ref, image_rows_ref, cap_sum_ref, region_sum_ref,
                       square_ref, out_grad_ref, cap_grad_out, region_grad_out, square_grad_out,
                       bias_out, pair_sc, image_acc, region_acc, weight_acc):
    step = pl.program_id(0)
    last = pl.num_programs(0) - 1
    slots, width = rows_ref.shape[1], rows_ref.shape[2]
    scaling = HEAD ** (-0.5)
    group = group_ref[step]
    half = lax.rem(step, 2)

    @pl.when(step == 0)
    def _():
        image_acc[...] = jnp.zeros_like(image_acc)
        region_acc[...] = jnp.zeros_like(region_acc)
        weight_acc[...] = jnp.zeros_like(weight_acc)
        bias_out[...] = jnp.zeros_like(bias_out)

    image_part = image_ref.at[group]
    cap_part = cap_ref.at[0]
    key_extra = key_mask_rows(length_ref[step], count_ref[step], slots)
    query_extra = query_mask_rows(slots)

    def heads(turn, carry):
        for inner in range(HEADS_AT_ONCE):
            head = turn * HEADS_AT_ONCE + inner
            query = head_rows(cap_part, image_part, head * HEAD)
            key = head_rows(cap_part, image_part, width + head * HEAD)
            value = head_rows(cap_part, image_part, 2 * width + head * HEAD)
            out_grad = context_grad_ref[0, pl.ds(pl.multiple_of(head * HEAD, HEAD), HEAD), :]
            scores = dot_tn(
                jnp.concatenate([key, key_extra], axis=0),
                jnp.concatenate([query, query_extra], axis=0),
            )
            probs = jnp.exp(scores - lse_ref[0, pl.ds(head, 1), :])
            probs_grad = dot_tn(value, out_grad)
            value_grad = dot_nt(out_grad, probs.astype(jnp.bfloat16))
            row_inner = jnp.sum(probs_grad * probs, axis=0, keepdims=True)
            score_grad = (probs * (probs_grad - row_inner)).astype(jnp.bfloat16)
            query_grad = dot_nn(key, score_grad) * scaling
            key_grad = dot_nt(query, score_grad)
            for part, grad in enumerate((query_grad, key_grad, value_grad)):
                rows = pl.ds(pl.multiple_of(part * width + head * HEAD, HEAD), HEAD)
                pair_sc[half, rows, :] = grad[:, :slots].astype(jnp.bfloat16)
                image_acc[group, rows, :] += grad[:, slots:]
        return carry

    lax.fori_loop(0, width // HEAD // HEADS_AT_ONCE, heads, 0)
    region_acc[group] += region_sum_ref[0]

    def flush(first, second, rows):
        for part in range(3):
            part_rows = slice(part * width, (part + 1) * width)
            pair = jnp.concatenate([first[part_rows, :], second[part_rows, :]], axis=1)
            weight_acc[part_rows, :] += dot_nn(pair, rows)
            bias_out[part_rows, :] += (
                first[part_rows, :].astype(jnp.float32) + second[part_rows, :].astype(jnp.float32)
            )
            product = dot_nn(square_ref[:, part_rows], pair)
            turned = product if part == 0 else turned + product
        return turned.T

    @pl.when(half == 1)
    def _():
        rows = rows_ref[...].reshape(2 * slots, width)
        grad = flush(pair_sc.at[0], pair_sc.at[1], rows)
        cap_grad_out[...] = cap_sum_ref[...] + grad.reshape(2, slots, width)

    @pl.when(step == last)
    def _():
        pair_sc[...] = image_acc[...].astype(jnp.bfloat16)
        rows = image_rows_ref[...].reshape(2 * slots, width)
        grad = flush(pair_sc.at[0], pair_sc.at[1], rows)
        region_grad_out[...] = region_acc[...] + grad.reshape(2, slots, width)
        square_grad_out[:, : 3 * width] = weight_acc[...].astype(jnp.bfloat16).T
        square_grad_out[:, 3 * width :] = out_grad_ref[...]


def attend_backward(lengths, counts, groups, cap_qkv, image_qkv, lse, context_grad, captions,
                    regions, cap_sum, region_sum, square, out_grad):
    seqs, slots, width = captions.shape
    images = regions.shape[0]
    heads = width // HEAD
    once = pl.Buffered(1)
    all_three = (images, slots, width)
    grid_spec = pltpu.PrefetchScalarGridSpec(
        num_scalar_prefetch=3,
        grid=(seqs,),
        in_specs=[
            pl.BlockSpec((1, 3 * width, slots), lambda s, *_: (s, 0, 0)),
            pl.BlockSpec((images, 3 * width, slots), lambda s, *_: (0, 0, 0), pipeline_mode=once),
            pl.BlockSpec((1, heads, 2 * slots), lambda s, *_: (s, 0, 0)),
            pl.BlockSpec((1, width, 2 * slots), lambda s, *_: (s, 0, 0)),
            pl.BlockSpec((2, slots, width), lambda s, *_: (s // 2, 0, 0)),
            pl.BlockSpec(all_three, lambda s, *_: (0, 0, 0), pipeline_mode=once),
            pl.BlockSpec((2, slots, width), lambda s, *_: (s // 2, 0, 0)),
            pl.BlockSpec((1, slots, width), lambda s, *_: (s, 0, 0)),
            pl.BlockSpec((width, 3 * width), lambda s, *_: (0, 0), pipeline_mode=once),
            pl.BlockSpec((width, width), lambda s, *_: (0, 0), pipeline_mode=once),
        ],
        out_specs=[
            pl.BlockSpec((2, slots, width), lambda s, *_: (s // 2, 0, 0)),
            pl.BlockSpec(all_three, lambda s, *_: (0, 0, 0), pipeline_mode=once),
            pl.BlockSpec((width, 4 * width), lambda s, *_: (0, 0), pipeline_mode=once),
            pl.BlockSpec((3 * width, 128), lambda s, *_: (0, 0), pipeline_mode=once),
        ],
        scratch_shapes=[
            pltpu.VMEM((2, 3 * width, slots), jnp.bfloat16),
            pltpu.VMEM((images, 3 * width, slots), jnp.float32),
            pltpu.VMEM(all_three, jnp.float32),
            pltpu.VMEM((3 * width, width), jnp.float32),
        ],
    )
    return pl.pallas_call(
        attend_back_kernel,
        grid_spec=grid_spec,
        out_shape=[
            jax.ShapeDtypeStruct((seqs, slots, width), jnp.float32),
            jax.ShapeDtypeStruct(all_three, jnp.float32),
            jax.ShapeDtypeStruct((width, 4 * width), jnp.bfloat16),
            jax.ShapeDtypeStruct((3 * width, 128), jnp.float32),
        ],
        compiler_params=pltpu.CompilerParams(vmem_limit_bytes=48 * 1024 * 1024),
        name="attend_backward",
    )(lengths, counts, groups, cap_qkv, image_qkv, lse, context_grad, captions, regions, cap_sum,
      region_sum, square, out_grad)


def on_device(
    use_kernels,
    captions,
    regions,
    caption_lengths,
    region_counts,
    group_ids,
    query_weight,
    key_weight,
    value_weight,
    out_weight,
    query_bias,
    value_bias,
    out_bias,
    first_gain,
    first_shift,
    inner_weight,
    inner_bias,
    outer_weight,
    outer_bias,
    second_gain,
    second_shift,
    caption_cotangent,
    region_cotangent,
):
    width = captions.shape[2]
    square, inner, outer, whole_vectors = gather_weights(
        (query_weight, key_weight, value_weight, out_weight),
        inner_weight,
        outer_weight,
        (
            query_bias,
            value_bias,
            out_bias,
            first_gain,
            first_shift,
            inner_bias,
            outer_bias,
            second_gain,
            second_shift,
        ),
        use_kernels,
    )
    wide = [vector.astype(jnp.float32) for vector in whole_vectors]
    query_all, value_all, out_all, gain_first, shift_first = wide[:5]
    inner_all, outer_all, gain_second, shift_second = wide[5:]
    bias_row = jnp.concatenate([query_all, jnp.zeros_like(query_all), value_all])[None, :]
    zero_row = jnp.zeros_like(out_all)
    vectors = jnp.stack(
        [out_all, gain_first, shift_first, outer_all, gain_second, shift_second, zero_row, zero_row]
    )
    seq_counts = jnp.sum(
        jnp.where(
            group_ids[:, None] == jnp.arange(regions.shape[0], dtype=jnp.int32)[None, :],
            region_counts[None, :],
            0,
        ),
        axis=1,
    )
    scalars = (caption_lengths, seq_counts, group_ids)
    cap_qkv, image_qkv, context, lse = attend_forward(
        *scalars, captions, regions, square, bias_row
    )
    (
        out_caption,
        out_region,
        cap_sum,
        region_sum,
        context_grad,
        out_grad,
        inner_grad,
        outer_grad,
        vector_grads,
        inner_bias_grad,
    ) = feed_both(
        *scalars,
        context,
        captions,
        regions,
        caption_cotangent,
        region_cotangent,
        square,
        inner,
        outer,
        vectors,
        inner_all[None, :],
    )
    grad_captions, grad_regions, square_grad, bias_wide = attend_backward(
        *scalars,
        cap_qkv,
        image_qkv,
        lse,
        context_grad,
        captions,
        regions,
        cap_sum,
        region_sum,
        square,
        out_grad,
    )
    bias_sums = jnp.sum(bias_wide, axis=1)
    square_total, inner_total, outer_total, vector_totals = reduce_weights(
        square_grad,
        inner_grad,
        outer_grad,
        (
            bias_sums[:width],
            bias_sums[2 * width :],
            vector_grads[0],
            vector_grads[1],
            vector_grads[2],
            inner_bias_grad[0],
            vector_grads[3],
            vector_grads[4],
            vector_grads[5],
        ),
        use_kernels,
    )
    return (
        out_caption,
        out_region,
        grad_captions,
        grad_regions,
        *jnp.split(square_total, 4, axis=1),
        *vector_totals[:5],
        inner_total,
        vector_totals[5],
        outer_total,
        *vector_totals[6:],
    )


def solution(mesh):
    use_kernels = mesh.shape["fsdp"] == OWNERS
    return jax.shard_map(
        functools.partial(on_device, use_kernels),
        mesh=mesh,
        in_specs=(
            P(("fsdp", "rep"), None, None),
            P(("fsdp", "rep"), None, None),
            P(("fsdp", "rep")),
            P(("fsdp", "rep")),
            P(("fsdp", "rep")),
            P("fsdp", None),
            P("fsdp", None),
            P("fsdp", None),
            P("fsdp", None),
            P("fsdp"),
            P("fsdp"),
            P("fsdp"),
            P("fsdp"),
            P("fsdp"),
            P("fsdp", None),
            P("fsdp"),
            P("fsdp", None),
            P("fsdp"),
            P("fsdp"),
            P("fsdp"),
            P(("fsdp", "rep"), None, None),
            P(("fsdp", "rep"), None, None),
        ),
        out_specs=(
            P(("fsdp", "rep"), None, None),
            P(("fsdp", "rep"), None, None),
            P(("fsdp", "rep"), None, None),
            P(("fsdp", "rep"), None, None),
            P("fsdp", None),
            P("fsdp", None),
            P("fsdp", None),
            P("fsdp", None),
            P("fsdp"),
            P("fsdp"),
            P("fsdp"),
            P("fsdp"),
            P("fsdp"),
            P("fsdp", None),
            P("fsdp"),
            P("fsdp", None),
            P("fsdp"),
            P("fsdp"),
            P("fsdp"),
        ),
        check_vma=False,
    )
```

```python
import functools

import jax
import jax.numpy as jnp
from jax import lax
from jax.experimental import pallas as pl
from jax.experimental.pallas import tpu as pltpu
from jax.sharding import PartitionSpec as P

EPSILON = 1e-12
MASKED_SCORE = -1e30

MESH = pl.DeviceIdType.MESH
PLANES = 4
COLUMN_SPLIT, ROW_SPLIT = 0, 1


def place_of(index, half, step, first, second):
    across = first * (1 - half) + second * half
    down = second * (1 - half) + first * half
    plane = lax.rem(index // 4 + step, PLANES)
    row = lax.rem(lax.rem(index // 2, 2) + down, 2)
    column = lax.rem(lax.rem(index, 2) + across, 2)
    return plane * 4 + row * 2 + column


def part_of(ref, split, owner, half, count, align):
    rows, columns = ref.shape[0] // count, ref.shape[1]
    if split == COLUMN_SPLIT:
        width = columns // 2
        return ref.at[
            pl.ds(pl.multiple_of(owner * rows, align), rows),
            pl.ds(pl.multiple_of(half * width, 128), width),
        ]
    height = rows // 2
    return ref.at[pl.ds(pl.multiple_of(owner * rows + half * height, align), height)]


def greet(index, half):
    barrier = pltpu.get_barrier_semaphore()
    peers = [(place_of(index, half, step, 0, 0), half) for step in (1, 2, 3)]
    peers += [(place_of(index, half, 0, 1, 0), half), (place_of(index, half, 0, 0, 1), half)]
    peers += [(index, 1 - half)]
    for peer in peers:
        pl.semaphore_signal(barrier, inc=1, device_id=peer, device_id_type=MESH)
    pl.semaphore_wait(barrier, len(peers))


def gather_phases(splits, aligns, shards, wholes, sems):
    count = len(splits)
    own_sem, z_send, z_recv, a_send, a_recv, b_send, b_recv, s_send, s_recv = sems
    index, half = lax.axis_index("fsdp"), lax.axis_index("rep")
    owners = wholes[0].shape[0] // shards[0].shape[0]

    def owner_of(step, first, second):
        return place_of(index, half, step, first, second)

    def piece(tensor, step, first, second):
        owner = owner_of(step, first, second)
        return part_of(wholes[tensor], splits[tensor], owner, half, owners, aligns[tensor])

    def copy_piece(tensor, source, step, first, second, send, recv, peer):
        return pltpu.make_async_remote_copy(
            src_ref=source,
            dst_ref=piece(tensor, step, first, second),
            send_sem=send,
            recv_sem=recv,
            device_id=peer,
            device_id_type=MESH,
        )

    def source_of(tensor, step, first, second):
        if step + first + second == 0:
            return part_of(shards[tensor], splits[tensor], 0, half, 1, aligns[tensor])
        return piece(tensor, step, first, second)

    peer_a = (owner_of(0, 1, 0), half)
    peer_b = (owner_of(0, 0, 1), half)
    sibling = (index, 1 - half)

    def to_z(tensor, hop):
        peer = (owner_of(hop, 0, 0), half)
        slot = PLANES - hop - 1
        source = source_of(tensor, 0, 0, 0)
        return copy_piece(
            tensor, source, 0, 0, 0, z_send.at[tensor, hop - 1], z_recv.at[tensor, slot], peer
        )

    def from_z(tensor, step):
        source = piece(tensor, step, 0, 0)
        return copy_piece(
            tensor,
            source,
            step,
            0,
            0,
            z_send.at[tensor, step - 1],
            z_recv.at[tensor, step - 1],
            sibling,
        )

    def to_a(tensor, step):
        source = source_of(tensor, step, 0, 0)
        return copy_piece(
            tensor, source, step, 0, 0, a_send.at[tensor, step], a_recv.at[tensor, step], peer_a
        )

    def from_a(tensor, step):
        source = piece(tensor, step, 1, 0)
        return copy_piece(
            tensor, source, step, 1, 0, a_send.at[tensor, step], a_recv.at[tensor, step], peer_a
        )

    def to_b(tensor, step, first):
        slot = step * 2 + first
        source = source_of(tensor, step, first, 0)
        return copy_piece(
            tensor, source, step, first, 0, b_send.at[tensor, slot], b_recv.at[tensor, slot], peer_b
        )

    def from_b(tensor, step, first):
        slot = step * 2 + first
        source = piece(tensor, step, first, 1)
        return copy_piece(
            tensor, source, step, first, 1, b_send.at[tensor, slot], b_recv.at[tensor, slot], peer_b
        )

    def to_sibling(tensor, step, first, second):
        slot = step * 4 + first * 2 + second - 1
        return copy_piece(
            tensor,
            piece(tensor, step, first, second),
            step,
            first,
            second,
            s_send.at[tensor, slot],
            s_recv.at[tensor, slot],
            sibling,
        )

    def from_sibling(tensor, step, first, second):
        slot = step * 4 + first * 2 + second - 1
        owner = place_of(index, 1 - half, step, first, second)
        there = part_of(wholes[tensor], splits[tensor], owner, 1 - half, owners, aligns[tensor])
        return pltpu.make_async_remote_copy(
            src_ref=there,
            dst_ref=there,
            send_sem=s_send.at[tensor, slot],
            recv_sem=s_recv.at[tensor, slot],
            device_id=sibling,
            device_id_type=MESH,
        )

    def own(tensor):
        rows = shards[tensor].shape[0]
        start = pl.multiple_of(index * rows, aligns[tensor])
        return pltpu.make_async_copy(
            shards[tensor], wholes[tensor].at[pl.ds(start, rows)], own_sem.at[tensor]
        )

    def start():
        greet(index, half)
        for tensor in range(count):
            for hop in (1, 2, 3):
                to_z(tensor, hop).start()
            to_a(tensor, 0).start()
            to_b(tensor, 0, 0).start()
            own(tensor).start()

    def pass_z(tensor, steps=(1, 2, 3)):
        for step in steps:
            from_z(tensor, step).wait_recv()
            to_b(tensor, step, 0).start()
            to_a(tensor, step).start()
            to_sibling(tensor, step, 0, 0).start()

    def pass_a(tensor, steps=(0, 1, 2, 3)):
        for step in steps:
            from_a(tensor, step).wait_recv()
            to_b(tensor, step, 1).start()
            to_sibling(tensor, step, 1, 0).start()

    def pass_b(tensor, steps=(0, 1, 2, 3), firsts=(0, 1)):
        for step in steps:
            for first in firsts:
                from_b(tensor, step, first).wait_recv()
                to_sibling(tensor, step, first, 1).start()

    def finish():
        for tensor in range(count):
            own(tensor).wait()
            for step in range(PLANES):
                for first in (0, 1):
                    for second in (0, 1):
                        if step + first + second == 0:
                            continue
                        from_sibling(tensor, step, first, second).wait_recv()
                        to_sibling(tensor, step, first, second).wait_send()
                    to_b(tensor, step, first).wait_send()
                to_a(tensor, step).wait_send()
                if step > 0:
                    to_z(tensor, step).wait_send()

    return start, pass_z, pass_a, pass_b, finish


def gather_kernel(splits, aligns, *refs):
    count = len(splits)
    start, pass_z, pass_a, pass_b, finish = gather_phases(
        splits, aligns, refs[:count], refs[count : 2 * count], refs[2 * count :]
    )
    start()
    for move in (pass_z, pass_a, pass_b):
        for tensor in range(count):
            move(tensor)
    finish()


def gather_semaphores(count):
    dma = pltpu.SemaphoreType.DMA
    return [
        dma((count,)),
        dma((count, 3)),
        dma((count, 3)),
        dma((count, 4)),
        dma((count, 4)),
        dma((count, 8)),
        dma((count, 8)),
        dma((count, 15)),
        dma((count, 15)),
    ]


def tile_rows(arrays):
    return [16 if array.dtype == jnp.bfloat16 else 8 for array in arrays]


def gather_all(shards, splits, owners, collective_id):
    count = len(shards)
    return pl.pallas_call(
        functools.partial(gather_kernel, splits, tile_rows(shards)),
        out_shape=[
            jax.ShapeDtypeStruct((owners * shard.shape[0], shard.shape[1]), shard.dtype)
            for shard in shards
        ],
        in_specs=[pl.BlockSpec(memory_space=pltpu.VMEM)] * count,
        out_specs=[pl.BlockSpec(memory_space=pl.ANY)] * count,
        scratch_shapes=gather_semaphores(count),
        compiler_params=pltpu.CompilerParams(collective_id=collective_id, has_side_effects=True),
        name="gather_rows",
    )(*shards)


def reduce_phases(splits, aligns, owners, partials, totals, buffers, sems):
    count = len(splits)
    mine, core_in, b_in, a_in, z_in = [
        buffers[kind * count : (kind + 1) * count] for kind in range(5)
    ]
    (load_sem, c_send, c_recv, b_send, b_recv, a_send, a_recv, z_send, z_recv, o_send, o_recv) = (
        sems
    )
    index, half = lax.axis_index("fsdp"), lax.axis_index("rep")
    sibling = (index, 1 - half)
    peer_a = (place_of(index, half, 0, 1, 0), half)
    peer_b = (place_of(index, half, 0, 0, 1), half)

    def slot_of(step, first, second):
        return second * 8 + first * 4 + step

    def load(tensor, step, first, second):
        owner = place_of(index, half, step, first, second)
        slot = slot_of(step, first, second)
        return pltpu.make_async_copy(
            part_of(partials[tensor], splits[tensor], owner, half, owners, aligns[tensor]),
            mine[tensor].at[slot],
            load_sem.at[tensor, slot],
        )

    def to_core(tensor, step, first, second):
        owner = place_of(index, 1 - half, step, first, second)
        slot = slot_of(step, first, second)
        return pltpu.make_async_remote_copy(
            src_ref=part_of(
                partials[tensor], splits[tensor], owner, 1 - half, owners, aligns[tensor]
            ),
            dst_ref=core_in[tensor].at[slot],
            send_sem=c_send.at[tensor, slot],
            recv_sem=c_recv.at[tensor, slot],
            device_id=sibling,
            device_id_type=MESH,
        )

    def to_b(tensor, step, first):
        slot = first * 4 + step
        return pltpu.make_async_remote_copy(
            src_ref=mine[tensor].at[8 + slot],
            dst_ref=b_in[tensor].at[slot],
            send_sem=b_send.at[tensor, slot],
            recv_sem=b_recv.at[tensor, slot],
            device_id=peer_b,
            device_id_type=MESH,
        )

    def to_a(tensor, step):
        return pltpu.make_async_remote_copy(
            src_ref=mine[tensor].at[4 + step],
            dst_ref=a_in[tensor].at[step],
            send_sem=a_send.at[tensor, step],
            recv_sem=a_recv.at[tensor, step],
            device_id=peer_a,
            device_id_type=MESH,
        )

    def to_z(tensor, hop):
        return pltpu.make_async_remote_copy(
            src_ref=mine[tensor].at[hop],
            dst_ref=z_in[tensor].at[PLANES - hop - 1],
            send_sem=z_send.at[tensor, hop - 1],
            recv_sem=z_recv.at[tensor, PLANES - hop - 1],
            device_id=(place_of(index, half, hop, 0, 0), half),
            device_id_type=MESH,
        )

    def wide(ref):
        return ref[...].astype(jnp.float32)

    def output_part(tensor):
        return part_of(totals[tensor], splits[tensor], 0, half, 1, 8)

    def to_output(tensor):
        return pltpu.make_async_remote_copy(
            src_ref=output_part(tensor),
            dst_ref=output_part(tensor),
            send_sem=o_send.at[tensor],
            recv_sem=o_recv.at[tensor],
            device_id=sibling,
            device_id_type=MESH,
        )

    def from_z(tensor, hop):
        slot = PLANES - hop - 1
        return pltpu.make_async_remote_copy(
            src_ref=mine[tensor].at[hop],
            dst_ref=z_in[tensor].at[slot],
            send_sem=z_send.at[tensor, hop - 1],
            recv_sem=z_recv.at[tensor, slot],
            device_id=sibling,
            device_id_type=MESH,
        )

    def from_output(tensor):
        there = part_of(totals[tensor], splits[tensor], 0, 1 - half, 1, 8)
        return pltpu.make_async_remote_copy(
            src_ref=there,
            dst_ref=there,
            send_sem=o_send.at[tensor],
            recv_sem=o_recv.at[tensor],
            device_id=sibling,
            device_id_type=MESH,
        )

    order = [(step, first, 1) for first in (1, 0) for step in (1, 2, 3, 0)]
    order += [(step, 1, 0) for step in (1, 2, 3, 0)] + [(step, 0, 0) for step in (1, 2, 3, 0)]

    def start():
        greet(index, half)
        for tensor in range(count):
            for step, first, second in order:
                to_core(tensor, step, first, second).start()
                load(tensor, step, first, second).start()

    def send_b(tensor):
        def turn_b(turn, carry):
            step, first = lax.rem(turn + 1, PLANES), 1 - turn // PLANES
            load(tensor, step, first, 1).wait()
            to_core(tensor, step, first, 1).wait_recv()
            slot = slot_of(step, first, 1)
            total = wide(mine[tensor].at[slot]) + wide(core_in[tensor].at[slot])
            mine[tensor].at[slot][...] = total.astype(mine[tensor].dtype)
            to_b(tensor, step, first).start()
            return carry

        lax.fori_loop(0, 2 * PLANES, turn_b, 0)

    def send_a(tensor):
        def turn_a(turn, carry):
            step = lax.rem(turn + 1, PLANES)
            load(tensor, step, 1, 0).wait()
            to_core(tensor, step, 1, 0).wait_recv()
            to_b(tensor, step, 1).wait_recv()
            slot = slot_of(step, 1, 0)
            total = wide(mine[tensor].at[slot]) + wide(core_in[tensor].at[slot])
            total += wide(b_in[tensor].at[slot])
            mine[tensor].at[slot][...] = total.astype(mine[tensor].dtype)
            to_a(tensor, step).start()
            return carry

        lax.fori_loop(0, PLANES, turn_a, 0)

    def send_z(tensor):
        def total_of(step):
            load(tensor, step, 0, 0).wait()
            to_core(tensor, step, 0, 0).wait_recv()
            to_b(tensor, step, 0).wait_recv()
            to_a(tensor, step).wait_recv()
            total = wide(mine[tensor].at[step]) + wide(core_in[tensor].at[step])
            return total + wide(b_in[tensor].at[step]) + wide(a_in[tensor].at[step])

        for hop in (1, 2, 3):
            mine[tensor].at[hop][...] = total_of(hop).astype(mine[tensor].dtype)
            to_z(tensor, hop).start()
        mine_total = total_of(0)
        output_part(tensor)[...] = mine_total

    def send_output(tensor):
        out = output_part(tensor)
        total = out[...]
        for hop in (1, 2, 3):
            from_z(tensor, hop).wait_recv()
            total += wide(z_in[tensor].at[PLANES - hop - 1])
        out[...] = total
        to_output(tensor).start()

    def finish():
        for tensor in range(count):
            from_output(tensor).wait_recv()
            to_output(tensor).wait_send()
            for step, first, second in order:
                to_core(tensor, step, first, second).wait_send()
                if second == 1:
                    to_b(tensor, step, first).wait_send()
                elif first == 1:
                    to_a(tensor, step).wait_send()
                elif step > 0:
                    to_z(tensor, step).wait_send()

    return start, send_b, send_a, send_z, send_output, finish


def reduce_kernel(splits, aligns, owners, *refs):
    count = len(splits)
    start, *moves, finish = reduce_phases(
        splits,
        aligns,
        owners,
        refs[:count],
        refs[count : 2 * count],
        refs[2 * count : 7 * count],
        refs[7 * count :],
    )
    start()
    for move in moves:
        for tensor in range(count):
            move(tensor)
    finish()


def reduce_scratch(partials, splits, owners):
    count = len(partials)
    dma = pltpu.SemaphoreType.DMA

    def pieces(slots):
        shapes = []
        for part, split in zip(partials, splits):
            rows, columns = part.shape[0] // owners, part.shape[1]
            shape = (rows, columns // 2) if split == COLUMN_SPLIT else (rows // 2, columns)
            shapes.append(pltpu.VMEM((slots, *shape), part.dtype))
        return shapes

    buffers = [*pieces(16), *pieces(16), *pieces(8), *pieces(4), *pieces(3)]
    sems = [
        dma((count, 16)),
        dma((count, 16)),
        dma((count, 16)),
        dma((count, 8)),
        dma((count, 8)),
        dma((count, 4)),
        dma((count, 4)),
        dma((count, 3)),
        dma((count, 3)),
        dma((count,)),
        dma((count,)),
    ]
    return buffers, sems


def reduce_all(partials, splits, owners, collective_id):
    count = len(partials)
    buffers, sems = reduce_scratch(partials, splits, owners)
    return pl.pallas_call(
        functools.partial(reduce_kernel, splits, tile_rows(partials), owners),
        out_shape=[
            jax.ShapeDtypeStruct((part.shape[0] // owners, part.shape[1]), jnp.float32)
            for part in partials
        ],
        in_specs=[pl.BlockSpec(memory_space=pl.ANY)] * count,
        out_specs=[pl.BlockSpec(memory_space=pltpu.VMEM)] * count,
        scratch_shapes=[*buffers, *sems],
        compiler_params=pltpu.CompilerParams(
            collective_id=collective_id, has_side_effects=True, vmem_limit_bytes=48 * 1024 * 1024
        ),
        name="reduce_rows",
    )(*partials)


OWNERS = 16
VECTOR_ROWS = 16
SQUARE_SPLITS = (COLUMN_SPLIT, ROW_SPLIT)
FEED_SPLITS = (COLUMN_SPLIT, ROW_SPLIT)


def pack_vectors(parts, owners):
    grid = jnp.concatenate([p.astype(jnp.float32).reshape(owners, -1) for p in parts], axis=1)
    grid = jnp.pad(grid, ((0, 0), (0, VECTOR_ROWS * 128 - grid.shape[1])))
    return grid.reshape(owners * VECTOR_ROWS, 128)


def unpack_vectors(rows, owners, sizes):
    grid = rows.reshape(owners, VECTOR_ROWS * 128)
    vectors, start = [], 0
    for size in sizes:
        vectors.append(grid[:, start : start + size].reshape(owners * size))
        start += size
    return vectors


def gather_weights(squares, vectors, use_kernels):
    square = jnp.concatenate(squares, axis=1)
    if not use_kernels:
        whole = [lax.all_gather(part, "fsdp", axis=0, tiled=True) for part in (square, *vectors)]
        return whole[0], whole[1:]
    packed = pack_vectors(vectors, 1)
    square, packed = gather_all((square, packed), SQUARE_SPLITS, OWNERS, 1)
    return square, unpack_vectors(packed, OWNERS, [v.shape[0] for v in vectors])


def reduce_native(part):
    share = lax.psum_scatter(part.astype(jnp.float32), "fsdp", scatter_dimension=0, tiled=True)
    return lax.psum(share.astype(jnp.bfloat16), "rep").astype(jnp.float32)


def reduce_weights(square, vectors, use_kernels):
    if not use_kernels:
        return reduce_native(square), [reduce_native(vector) for vector in vectors]
    packed = pack_vectors(vectors, OWNERS)
    square, packed = reduce_all((square, packed), SQUARE_SPLITS, OWNERS, 2)
    return square, unpack_vectors(packed, 1, [v.shape[0] // OWNERS for v in vectors])


def dot_nn(left, right):
    return lax.dot_general(
        left, right, (((1,), (0,)), ((), ())), preferred_element_type=jnp.float32
    )


def dot_nt(left, right):
    return lax.dot_general(
        left, right, (((1,), (1,)), ((), ())), preferred_element_type=jnp.float32
    )


def dot_tn(left, right):
    return lax.dot_general(
        left, right, (((0,), (0,)), ((), ())), preferred_element_type=jnp.float32
    )


HEAD = 64
EXTRA_ROWS = 16
HEADS_AT_ONCE = 2


def key_mask_rows(length, count, slots):
    slot = lax.broadcasted_iota(jnp.int32, (EXTRA_ROWS, 2 * slots), 1)
    row = lax.broadcasted_iota(jnp.int32, (EXTRA_ROWS, 2 * slots), 0)
    live = (slot < length) | ((slot >= slots) & (slot < slots + count))
    return jnp.where((row > 0) | live, 0.0, MASKED_SCORE).astype(jnp.bfloat16)


def query_mask_rows(slots):
    row = lax.broadcasted_iota(jnp.int32, (EXTRA_ROWS, 2 * slots), 0)
    return jnp.where(row == 0, 1.0, 0.0).astype(jnp.bfloat16)


def live_rows_column(length, count, slots):
    row = lax.broadcasted_iota(jnp.int32, (2 * slots, 1), 0)
    live = (row < length) | ((row >= slots) & (row < slots + count))
    return jnp.where(live, 1.0, 0.0)


def head_rows(cap_part, image_part, base):
    rows = pl.ds(pl.multiple_of(base, HEAD), HEAD)
    return jnp.concatenate([cap_part[rows, :], image_part[rows, :]], axis=1)


def project_kernel(share, length_ref, count_ref, group_ref, cap_ref, image_ref, weight_ref,
                   bias_ref, *refs):
    shards, refs = refs[:share], refs[share:]
    (cap_out, image_out, context_out, lse_out), refs = refs[:4], refs[4:]
    wholes, refs = refs[:share], refs[share:]
    (weight_turned, bias_wide), sems = refs[:2], refs[2:]
    step = pl.program_id(0)
    if share:
        start, pass_z, pass_a, pass_b, finish = gather_phases(
            FEED_SPLITS, tile_rows(shards), shards, wholes, sems
        )
        later = (1, 2, 3)

        @pl.when(step == 0)
        def _():
            start()

        @pl.when(step == 1)
        def _():
            pass_a(0, (0,))
            pass_a(1, (0,))
            pass_z(0)

        @pl.when(step == 2)
        def _():
            pass_a(0, later)

        @pl.when(step == 3)
        def _():
            pass_z(1)
            pass_b(0, (0,))

        @pl.when(step == 4)
        def _():
            pass_a(1, later)
            pass_b(1, (0,))

        for turn, (tensor, first) in enumerate(((0, 0), (0, 1), (1, 0), (1, 1))):

            @pl.when(step == 5 + turn)
            def _(tensor=tensor, first=first):
                pass_b(tensor, later, (first,))

    width = cap_ref.shape[2]
    slots = cap_ref.shape[1]
    scaling = HEAD ** (-0.5)

    @pl.when(step == 0)
    def _():
        weight_turned[...] = weight_ref[:, : 3 * width].T
        bias_wide[...] = jnp.broadcast_to(bias_ref[...], (128, 3 * width)).T

    def project(rows):
        parts = []
        for part in range(3):
            turned = dot_nt(weight_turned[part * width : (part + 1) * width, :], rows)
            bias = bias_wide[part * width : (part + 1) * width, :]
            turned = turned + jnp.concatenate([bias, bias], axis=1)
            turned = turned.astype(jnp.bfloat16)
            parts.append(turned * scaling if part == 0 else turned)
        return parts

    @pl.when(step == 0)
    def _():
        parts = project(image_ref[...].reshape(2 * slots, width))
        for part in range(3):
            rows = slice(part * width, (part + 1) * width)
            image_out[0, rows, :] = parts[part][:, :slots]
            image_out[1, rows, :] = parts[part][:, slots:]

    @pl.when(lax.rem(step, 2) == 0)
    def _():
        parts = project(cap_ref[...].reshape(2 * slots, width))
        for part in range(3):
            rows = slice(part * width, (part + 1) * width)
            cap_out[0, rows, :] = parts[part][:, :slots]
            cap_out[1, rows, :] = parts[part][:, slots:]

    cap_part = cap_out.at[lax.rem(step, 2)]
    image_part = image_out.at[group_ref[step]]
    key_extra = key_mask_rows(length_ref[step], count_ref[step], slots)
    query_extra = query_mask_rows(slots)

    def heads(turn, carry):
        for inner in range(HEADS_AT_ONCE):
            head = turn * HEADS_AT_ONCE + inner
            query = head_rows(cap_part, image_part, head * HEAD)
            key = head_rows(cap_part, image_part, width + head * HEAD)
            value = head_rows(cap_part, image_part, 2 * width + head * HEAD)
            scores = dot_tn(
                jnp.concatenate([key, key_extra], axis=0),
                jnp.concatenate([query, query_extra], axis=0),
            )
            largest = jnp.max(scores, axis=0, keepdims=True)
            powers = jnp.exp(scores - largest)
            total = jnp.sum(powers, axis=0, keepdims=True)
            probs = (powers * (1.0 / total)).astype(jnp.bfloat16)
            context = dot_nn(value, probs)
            context_out[0, pl.ds(pl.multiple_of(head * HEAD, HEAD), HEAD), :] = context.astype(
                jnp.bfloat16
            )
            lse_out[0, pl.ds(head, 1), :] = largest + jnp.log(total)
        return carry

    lax.fori_loop(0, width // HEAD // HEADS_AT_ONCE, heads, 0)
    if share:

        @pl.when(step == pl.num_programs(0) - 1)
        def _():
            finish()


SCALARS = [pl.BlockSpec(memory_space=pltpu.SMEM)] * 3


def attend_forward(lengths, counts, groups, captions, regions, square, bias_row, shards):
    seqs, slots, width = captions.shape
    images = regions.shape[0]
    heads = width // HEAD
    share = len(shards)
    params = {"collective_id": 3, "has_side_effects": True} if share else {}
    low, wide = jnp.bfloat16, jnp.float32
    anywhere = [pl.BlockSpec(memory_space=pl.ANY)] * share
    return pl.pallas_call(
        functools.partial(project_kernel, share),
        grid=(seqs,),
        in_specs=[
            *SCALARS,
            pl.BlockSpec((2, slots, width), lambda s: (s // 2, 0, 0)),
            pl.BlockSpec((images, slots, width), lambda s: (0, 0, 0)),
            pl.BlockSpec(square.shape, lambda s: (0, 0), pipeline_mode=pl.Buffered(1)),
            pl.BlockSpec(bias_row.shape, lambda s: (0, 0)),
            *anywhere,
        ],
        out_specs=[
            pl.BlockSpec((2, 3 * width, slots), lambda s: (s // 2, 0, 0)),
            pl.BlockSpec((images, 3 * width, slots), lambda s: (0, 0, 0)),
            pl.BlockSpec((1, width, 2 * slots), lambda s: (s, 0, 0)),
            pl.BlockSpec((1, heads, 2 * slots), lambda s: (s, 0, 0)),
            *anywhere,
        ],
        scratch_shapes=[
            pltpu.VMEM((3 * width, width), low),
            pltpu.VMEM((3 * width, 128), wide),
            *(gather_semaphores(share) if share else ()),
        ],
        out_shape=[
            jax.ShapeDtypeStruct((seqs, 3 * width, slots), low),
            jax.ShapeDtypeStruct((images, 3 * width, slots), low),
            jax.ShapeDtypeStruct((seqs, width, 2 * slots), low),
            jax.ShapeDtypeStruct((seqs, heads, 2 * slots), wide),
            *[
                jax.ShapeDtypeStruct((OWNERS * shard.shape[0], shard.shape[1]), shard.dtype)
                for shard in shards
            ],
        ],
        compiler_params=pltpu.CompilerParams(vmem_limit_bytes=48 * 1024 * 1024, **params),
        name="attend_forward",
    )(lengths, counts, groups, captions, regions, square, bias_row, *shards)


PHI_SLOPE = 0.2316419
PHI_TERMS = (0.319381530, -0.356563782, 1.781477937, -1.821255978, 1.330274429)
FF_CHUNK = 512


def gelu_both(values):
    density = 0.3989422804014327 * jnp.exp(-0.5 * values * values)
    ratio = 1.0 / (1.0 + PHI_SLOPE * jnp.abs(values))
    tail = PHI_TERMS[4]
    for term in PHI_TERMS[3::-1]:
        tail = tail * ratio + term
    tail = tail * ratio * density
    below = jnp.where(values >= 0.0, 1.0 - tail, tail)
    return values * below, below + values * density


def norm_parts(values):
    average = jnp.mean(values, axis=-1, keepdims=True)
    centred = values - average
    spread = jnp.mean(centred * centred, axis=-1, keepdims=True)
    inverse = lax.rsqrt(spread + EPSILON)
    return centred * inverse, inverse


def norm_back(gradient, gain, normal, inverse):
    scaled = gradient * gain
    first = jnp.mean(scaled, axis=-1, keepdims=True)
    second = jnp.mean(scaled * normal, axis=-1, keepdims=True)
    return (scaled - first - normal * second) * inverse


def feed_kernel(length_ref, count_ref, group_ref, context_ref, cap_ref, image_ref, cap_cot_ref,
                region_cot_ref, out_weight_ref, inner_ref, outer_ref, vector_ref, inner_bias_ref,
                out_cap_ref, out_region_ref, cap_sum_ref, region_sum_ref, context_grad_ref,
                out_grad_ref, inner_grad_ref, outer_grad_ref, vector_grad_ref, bias_grad_ref,
                active_sc, slope_sc, inner_acc, outer_acc, out_acc):
    step = pl.program_id(0)
    slots = cap_ref.shape[1]
    hidden = inner_ref.shape[1]
    chunks = [slice(start, start + FF_CHUNK) for start in range(0, hidden, FF_CHUNK)]

    @pl.when(step == 0)
    def _():
        inner_acc[...] = jnp.zeros_like(inner_acc)
        outer_acc[...] = jnp.zeros_like(outer_acc)
        out_acc[...] = jnp.zeros_like(out_acc)
        vector_grad_ref[...] = jnp.zeros_like(vector_grad_ref)
        bias_grad_ref[...] = jnp.zeros_like(bias_grad_ref)

    def vector(row):
        return vector_ref[row : row + 1, :]

    def add_vector(row, values):
        vector_grad_ref[row : row + 1, :] += jnp.sum(values, axis=0, keepdims=True)

    live = live_rows_column(length_ref[step], count_ref[step], slots)
    rows_in = jnp.concatenate([cap_ref[0], image_ref[0]], axis=0).astype(jnp.float32)
    first_sum = rows_in + dot_tn(context_ref[0], out_weight_ref[...]) + vector(0)
    first_normal, first_inverse = norm_parts(first_sum)
    first_out = first_normal * vector(1) + vector(2)
    first_low = first_out.astype(jnp.bfloat16)
    second_sum = first_out + vector(3)
    for chunk in chunks:
        pre = dot_nn(first_low, inner_ref[:, chunk]) + inner_bias_ref[:, chunk]
        active, slope = gelu_both(pre)
        active = active.astype(jnp.bfloat16)
        active_sc[:, chunk] = active
        slope_sc[:, chunk] = slope
        second_sum = second_sum + dot_nn(active, outer_ref[chunk, :])
    second_normal, second_inverse = norm_parts(second_sum)
    result = ((second_normal * vector(4) + vector(5)) * live).astype(jnp.bfloat16)
    out_cap_ref[0] = result[:slots]
    out_region_ref[0] = result[slots:]
    cot = jnp.concatenate([cap_cot_ref[0], region_cot_ref[0]], axis=0).astype(jnp.float32) * live
    add_vector(4, cot * second_normal)
    add_vector(5, cot)
    second_grad = norm_back(cot, vector(4), second_normal, second_inverse)
    outer_grad = second_grad.astype(jnp.bfloat16)
    add_vector(3, outer_grad.astype(jnp.float32))
    first_grad = second_grad
    first_turned = first_low.T
    for chunk in chunks:
        active_grad = dot_nt(outer_grad, outer_ref[chunk, :])
        inner_grad = (active_grad * slope_sc[:, chunk]).astype(jnp.bfloat16)
        bias_grad_ref[:, chunk] += jnp.sum(inner_grad.astype(jnp.float32), axis=0, keepdims=True)
        inner_acc[:, chunk] += dot_nn(first_turned, inner_grad)
        outer_acc[chunk, :] += dot_tn(active_sc[:, chunk], outer_grad)
        first_grad = first_grad + dot_nt(inner_grad, inner_ref[:, chunk])
    add_vector(1, first_grad * first_normal)
    add_vector(2, first_grad)
    sum_grad = norm_back(first_grad, vector(1), first_normal, first_inverse)
    cap_sum_ref[0] = sum_grad[:slots]
    region_sum_ref[0] = sum_grad[slots:]
    attended_grad = sum_grad.astype(jnp.bfloat16)
    add_vector(0, attended_grad.astype(jnp.float32))
    out_acc[...] += dot_nn(context_ref[0], attended_grad)
    context_grad_ref[0] = dot_nt(out_weight_ref[...], attended_grad).astype(jnp.bfloat16)

    @pl.when(step == pl.num_programs(0) - 1)
    def _():
        out_grad_ref[...] = out_acc[...].astype(jnp.bfloat16)
        inner_grad_ref[...] = inner_acc[...].astype(jnp.bfloat16)
        outer_grad_ref[...] = outer_acc[...].astype(jnp.bfloat16)


def feed_both(lengths, counts, groups, context, captions, regions, cap_cot, region_cot, square,
              inner, outer, vectors, inner_bias):
    seqs, slots, width = captions.shape
    hidden = inner.shape[1]
    once = pl.Buffered(1)

    def seq_block(*shape):
        return pl.BlockSpec((1, *shape), lambda s, *_: (s, 0, 0))

    def whole(shape, column=0):
        return pl.BlockSpec(shape, lambda s, *_: (0, column), pipeline_mode=once)

    grid_spec = pltpu.PrefetchScalarGridSpec(
        num_scalar_prefetch=3,
        grid=(seqs,),
        in_specs=[
            seq_block(width, 2 * slots),
            seq_block(slots, width),
            pl.BlockSpec((1, slots, width), lambda s, lens, counts, group: (group[s], 0, 0)),
            seq_block(slots, width),
            seq_block(slots, width),
            whole((width, width), 3),
            whole((width, hidden)),
            whole((hidden, width)),
            whole(vectors.shape),
            whole(inner_bias.shape),
        ],
        out_specs=[
            seq_block(slots, width),
            seq_block(slots, width),
            seq_block(slots, width),
            seq_block(slots, width),
            seq_block(width, 2 * slots),
            whole((width, width)),
            whole((width, hidden)),
            whole((hidden, width)),
            whole((8, width)),
            whole((1, hidden)),
        ],
        scratch_shapes=[
            pltpu.VMEM((2 * slots, hidden), jnp.bfloat16),
            pltpu.VMEM((2 * slots, hidden), jnp.float32),
            pltpu.VMEM((width, hidden), jnp.float32),
            pltpu.VMEM((hidden, width), jnp.float32),
            pltpu.VMEM((width, width), jnp.float32),
        ],
    )
    low, wide = jnp.bfloat16, jnp.float32
    rows_shape = (seqs, slots, width)
    return pl.pallas_call(
        feed_kernel,
        grid_spec=grid_spec,
        out_shape=[
            jax.ShapeDtypeStruct(rows_shape, low),
            jax.ShapeDtypeStruct(rows_shape, low),
            jax.ShapeDtypeStruct(rows_shape, wide),
            jax.ShapeDtypeStruct(rows_shape, wide),
            jax.ShapeDtypeStruct((seqs, width, 2 * slots), low),
            jax.ShapeDtypeStruct((width, width), low),
            jax.ShapeDtypeStruct((width, hidden), low),
            jax.ShapeDtypeStruct((hidden, width), low),
            jax.ShapeDtypeStruct((8, width), wide),
            jax.ShapeDtypeStruct((1, hidden), wide),
        ],
        compiler_params=pltpu.CompilerParams(vmem_limit_bytes=63 * 1024 * 1024),
        name="feed_both",
    )(lengths, counts, groups, context, captions, regions, cap_cot, region_cot, square, inner,
      outer, vectors, inner_bias)


def attend_back_kernel(share, length_ref, count_ref, group_ref, cap_ref, image_ref, lse_ref,
                       context_grad_ref, rows_ref, image_rows_ref, cap_sum_ref, region_sum_ref,
                       square_ref, out_grad_ref, *refs):
    partials, refs = refs[:share], refs[share:]
    (cap_grad_out, region_grad_out, square_grad_out, bias_out), refs = refs[:4], refs[4:]
    total_outs, refs = refs[:share], refs[share:]
    (pair_sc, image_acc, region_acc, weight_acc), refs = refs[:4], refs[4:]
    totals, buffers, sems = refs[:share], refs[share : 6 * share], refs[6 * share :]
    step = pl.program_id(0)
    last = pl.num_programs(0) - 1
    images = image_ref.shape[0]
    if share:
        start, send_b, send_a, send_z, send_output, finish = reduce_phases(
            FEED_SPLITS, tile_rows(partials), OWNERS, partials, totals, buffers, sems
        )

        @pl.when(step == 0)
        def _():
            start()

        schedule = ((1, send_b, 0), (2, send_b, 1), (4, send_a, 0), (5, send_a, 1))
        schedule += ((6, send_z, 0), (7, send_z, 1), (8, send_output, 0))
        for when, move, tensor in schedule:

            @pl.when(step == when)
            def _(move=move, tensor=tensor):
                move(tensor)

    slots, width = rows_ref.shape[1], rows_ref.shape[2]
    scaling = HEAD ** (-0.5)
    group = group_ref[step]
    half = lax.rem(step, 2)

    @pl.when(step == 0)
    def _():
        image_acc[...] = jnp.zeros_like(image_acc)
        region_acc[...] = jnp.zeros_like(region_acc)
        weight_acc[...] = jnp.zeros_like(weight_acc)
        bias_out[...] = jnp.zeros_like(bias_out)

    image_part = image_ref.at[group]
    uses = [(group == image).astype(jnp.float32) for image in range(images)]
    cap_part = cap_ref.at[0]
    key_extra = key_mask_rows(length_ref[step], count_ref[step], slots)
    query_extra = query_mask_rows(slots)

    def heads(turn, carry):
        for inner in range(HEADS_AT_ONCE):
            head = turn * HEADS_AT_ONCE + inner
            query = head_rows(cap_part, image_part, head * HEAD)
            key = head_rows(cap_part, image_part, width + head * HEAD)
            value = head_rows(cap_part, image_part, 2 * width + head * HEAD)
            out_grad = context_grad_ref[0, pl.ds(pl.multiple_of(head * HEAD, HEAD), HEAD), :]
            scores = dot_tn(
                jnp.concatenate([key, key_extra], axis=0),
                jnp.concatenate([query, query_extra], axis=0),
            )
            probs = jnp.exp(scores - lse_ref[0, pl.ds(head, 1), :])
            probs_grad = dot_tn(value, out_grad)
            value_grad = dot_nt(out_grad, probs.astype(jnp.bfloat16))
            row_inner = jnp.sum(probs_grad * probs, axis=0, keepdims=True)
            score_grad = (probs * (probs_grad - row_inner)).astype(jnp.bfloat16)
            query_grad = dot_nn(key, score_grad) * scaling
            key_grad = dot_nt(query, score_grad)
            for part, grad in enumerate((query_grad, key_grad, value_grad)):
                rows = pl.ds(pl.multiple_of(part * width + head * HEAD, HEAD), HEAD)
                pair_sc[half, rows, :] = grad[:, :slots].astype(jnp.bfloat16)
                for image in range(images):
                    image_acc[image, rows, :] += grad[:, slots:] * uses[image]
        return carry

    lax.fori_loop(0, width // HEAD // HEADS_AT_ONCE, heads, 0)
    for image in range(images):
        region_acc[image] += region_sum_ref[0] * uses[image]

    def flush(first, second, rows):
        for part in range(3):
            part_rows = slice(part * width, (part + 1) * width)
            pair = jnp.concatenate([first[part_rows, :], second[part_rows, :]], axis=1)
            weight_acc[part_rows, :] += dot_nn(pair, rows)
            bias_out[part_rows, :] += (
                first[part_rows, :].astype(jnp.float32) + second[part_rows, :].astype(jnp.float32)
            )
            product = dot_nn(square_ref[:, part_rows], pair)
            turned = product if part == 0 else turned + product
        return turned.T

    @pl.when(half == 1)
    def _():
        rows = rows_ref[...].reshape(2 * slots, width)
        grad = flush(pair_sc.at[0], pair_sc.at[1], rows)
        cap_grad_out[...] = cap_sum_ref[...] + grad.reshape(2, slots, width)

    @pl.when(step == last)
    def _():
        pair_sc[...] = image_acc[...].astype(jnp.bfloat16)
        rows = image_rows_ref[...].reshape(2 * slots, width)
        grad = flush(pair_sc.at[0], pair_sc.at[1], rows)
        region_grad_out[...] = region_acc[...] + grad.reshape(2, slots, width)
        square_grad_out[:, : 3 * width] = weight_acc[...].astype(jnp.bfloat16).T
        square_grad_out[:, 3 * width :] = out_grad_ref[...]
        if share:
            send_output(1)
            finish()
            for out, total in zip(total_outs, totals):
                out[...] = total[...]


def attend_backward(lengths, counts, groups, cap_qkv, image_qkv, lse, context_grad, captions,
                    regions, cap_sum, region_sum, square, out_grad, partials):
    seqs, slots, width = captions.shape
    images = regions.shape[0]
    heads = width // HEAD
    share = len(partials)
    params = {"collective_id": 4, "has_side_effects": True} if share else {}
    once = pl.Buffered(1)
    low, wide = jnp.bfloat16, jnp.float32
    all_three = (images, slots, width)
    shapes = [(part.shape[0] // OWNERS, part.shape[1]) for part in partials]
    buffers, sems = reduce_scratch(partials, FEED_SPLITS, OWNERS) if share else ((), ())

    def whole(*shape):
        return pl.BlockSpec(shape, lambda s: (0,) * len(shape), pipeline_mode=once)

    return pl.pallas_call(
        functools.partial(attend_back_kernel, share),
        grid=(seqs,),
        in_specs=[
            *SCALARS,
            pl.BlockSpec((1, 3 * width, slots), lambda s: (s, 0, 0)),
            whole(images, 3 * width, slots),
            pl.BlockSpec((1, heads, 2 * slots), lambda s: (s, 0, 0)),
            pl.BlockSpec((1, width, 2 * slots), lambda s: (s, 0, 0)),
            pl.BlockSpec((2, slots, width), lambda s: (s // 2, 0, 0)),
            whole(*all_three),
            pl.BlockSpec((2, slots, width), lambda s: (s // 2, 0, 0)),
            pl.BlockSpec((1, slots, width), lambda s: (s, 0, 0)),
            whole(width, 3 * width),
            whole(width, width),
            *[pl.BlockSpec(memory_space=pl.ANY)] * share,
        ],
        out_specs=[
            pl.BlockSpec((2, slots, width), lambda s: (s // 2, 0, 0)),
            whole(*all_three),
            whole(width, 4 * width),
            whole(3 * width, 128),
            *[whole(*shape) for shape in shapes],
        ],
        scratch_shapes=[
            pltpu.VMEM((2, 3 * width, slots), low),
            pltpu.VMEM((images, 3 * width, slots), wide),
            pltpu.VMEM(all_three, wide),
            pltpu.VMEM((3 * width, width), wide),
            *[pltpu.VMEM(shape, wide) for shape in shapes],
            *buffers,
            *sems,
        ],
        out_shape=[
            jax.ShapeDtypeStruct((seqs, slots, width), wide),
            jax.ShapeDtypeStruct(all_three, wide),
            jax.ShapeDtypeStruct((width, 4 * width), low),
            jax.ShapeDtypeStruct((3 * width, 128), wide),
            *[jax.ShapeDtypeStruct(shape, wide) for shape in shapes],
        ],
        compiler_params=pltpu.CompilerParams(vmem_limit_bytes=62 * 1024 * 1024, **params),
        name="attend_backward",
    )(lengths, counts, groups, cap_qkv, image_qkv, lse, context_grad, captions, regions, cap_sum,
      region_sum, square, out_grad, *partials)


def on_device(
    use_kernels,
    captions,
    regions,
    caption_lengths,
    region_counts,
    group_ids,
    query_weight,
    key_weight,
    value_weight,
    out_weight,
    query_bias,
    value_bias,
    out_bias,
    first_gain,
    first_shift,
    inner_weight,
    inner_bias,
    outer_weight,
    outer_bias,
    second_gain,
    second_shift,
    caption_cotangent,
    region_cotangent,
):
    width = captions.shape[2]
    square, whole_vectors = gather_weights(
        (query_weight, key_weight, value_weight, out_weight),
        (
            query_bias,
            value_bias,
            out_bias,
            first_gain,
            first_shift,
            inner_bias,
            outer_bias,
            second_gain,
            second_shift,
        ),
        use_kernels,
    )
    wide = [vector.astype(jnp.float32) for vector in whole_vectors]
    query_all, value_all, out_all, gain_first, shift_first = wide[:5]
    inner_all, outer_all, gain_second, shift_second = wide[5:]
    bias_row = jnp.concatenate([query_all, jnp.zeros_like(query_all), value_all])[None, :]
    zero_row = jnp.zeros_like(out_all)
    vectors = jnp.stack(
        [out_all, gain_first, shift_first, outer_all, gain_second, shift_second, zero_row, zero_row]
    )
    seq_counts = jnp.sum(
        jnp.where(
            group_ids[:, None] == jnp.arange(regions.shape[0], dtype=jnp.int32)[None, :],
            region_counts[None, :],
            0,
        ),
        axis=1,
    )
    scalars = (caption_lengths, seq_counts, group_ids)
    shards = (inner_weight, outer_weight)
    cap_qkv, image_qkv, context, lse, *wholes = attend_forward(
        *scalars, captions, regions, square, bias_row, shards if use_kernels else ()
    )
    if not use_kernels:
        wholes = [lax.all_gather(shard, "fsdp", axis=0, tiled=True) for shard in shards]
    inner, outer = wholes
    (
        out_caption,
        out_region,
        cap_sum,
        region_sum,
        context_grad,
        out_grad,
        inner_grad,
        outer_grad,
        vector_grads,
        inner_bias_grad,
    ) = feed_both(
        *scalars,
        context,
        captions,
        regions,
        caption_cotangent,
        region_cotangent,
        square,
        inner,
        outer,
        vectors,
        inner_all[None, :],
    )
    grad_captions, grad_regions, square_grad, bias_wide, *totals = attend_backward(
        *scalars,
        cap_qkv,
        image_qkv,
        lse,
        context_grad,
        captions,
        regions,
        cap_sum,
        region_sum,
        square,
        out_grad,
        (inner_grad, outer_grad) if use_kernels else (),
    )
    if not use_kernels:
        totals = [reduce_native(part) for part in (inner_grad, outer_grad)]
    inner_total, outer_total = totals
    bias_sums = jnp.sum(bias_wide, axis=1)
    square_total, vector_totals = reduce_weights(
        square_grad,
        (
            bias_sums[:width],
            bias_sums[2 * width :],
            vector_grads[0],
            vector_grads[1],
            vector_grads[2],
            inner_bias_grad[0],
            vector_grads[3],
            vector_grads[4],
            vector_grads[5],
        ),
        use_kernels,
    )
    return (
        out_caption,
        out_region,
        grad_captions,
        grad_regions,
        *jnp.split(square_total, 4, axis=1),
        *vector_totals[:5],
        inner_total,
        vector_totals[5],
        outer_total,
        *vector_totals[6:],
    )


def solution(mesh):
    use_kernels = mesh.shape["fsdp"] == OWNERS
    return jax.shard_map(
        functools.partial(on_device, use_kernels),
        mesh=mesh,
        in_specs=(
            P(("fsdp", "rep"), None, None),
            P(("fsdp", "rep"), None, None),
            P(("fsdp", "rep")),
            P(("fsdp", "rep")),
            P(("fsdp", "rep")),
            P("fsdp", None),
            P("fsdp", None),
            P("fsdp", None),
            P("fsdp", None),
            P("fsdp"),
            P("fsdp"),
            P("fsdp"),
            P("fsdp"),
            P("fsdp"),
            P("fsdp", None),
            P("fsdp"),
            P("fsdp", None),
            P("fsdp"),
            P("fsdp"),
            P("fsdp"),
            P(("fsdp", "rep"), None, None),
            P(("fsdp", "rep"), None, None),
        ),
        out_specs=(
            P(("fsdp", "rep"), None, None),
            P(("fsdp", "rep"), None, None),
            P(("fsdp", "rep"), None, None),
            P(("fsdp", "rep"), None, None),
            P("fsdp", None),
            P("fsdp", None),
            P("fsdp", None),
            P("fsdp", None),
            P("fsdp"),
            P("fsdp"),
            P("fsdp"),
            P("fsdp"),
            P("fsdp"),
            P("fsdp", None),
            P("fsdp"),
            P("fsdp", None),
            P("fsdp"),
            P("fsdp"),
            P("fsdp"),
        ),
        check_vma=False,
    )
```
